32 devices in a mesh: dp: 2 (over x), context: 4 (over z), experts: 4 (over y, core).
Axes of the slice: x: 2, y: 2, z: 4, core: 2. Of those that a mesh axis runs over, the one named last changes fastest.
Arguments:
- layer_input: bfloat16 [2, 2048, 2048], P('dp', ('context', 'experts')), may hold values from -6 to 6
- cotangent: bfloat16 [2, 2048, 2048], P('dp', ('context', 'experts')), may hold values from -6 to 6
- routes: int32 [2, 2048, 6], P('dp', ('context', 'experts')), may hold values from 0 to 15, all different within a row; in each aligned block of 128 rows (0 to 127, 128 to 255, ..., all dimensions but the last counted through in order) at most 64 rows name the same one
- span_order: int32 [8], replicated, may hold values from 0 to 7, each once
- attn_gain: bfloat16 [2048], P('dp'), may hold values from 0.5 to 1.5
- query_proj: bfloat16 [2048, 3072], P('dp', 'experts'), may hold values from -0.125 to 0.125
- latent_proj: bfloat16 [2048, 576], P('dp'), may hold values from -0.125 to 0.125
- latent_gain: bfloat16 [512], P('dp'), may hold values from 0.5 to 1.5
- expand_proj: bfloat16 [512, 4096], P('dp', 'experts'), may hold values from -0.25 to 0.25
- output_proj: bfloat16 [2048, 2048], P('experts', 'dp'), may hold values from -0.375 to 0.375
- moe_gain: bfloat16 [2048], P('dp'), may hold values from 0.5 to 1.5
- router_proj: bfloat16 [2048, 16], P('dp'), may hold values from -0.25 to 0.25
- shared_in: bfloat16 [2048, 2, 2816], P('dp', None, 'experts'), may hold values from -0.125 to 0.125
- shared_out: bfloat16 [2816, 2048], P('experts', 'dp'), may hold values from -0.109375 to 0.109375
- expert_in: bfloat16 [16, 2048, 2, 1408], P(('context', 'experts'), None, None, 'dp'), may hold values from -0.125 to 0.125
- expert_out: bfloat16 [16, 1408, 2048], P(('context', 'experts'), 'dp'), may hold values from -0.15625 to 0.15625
Outputs:
- block_output: float32 [2, 2048, 2048], P('dp', ('context', 'experts'))
- input_grad: float32 [2, 2048, 2048], P('dp', ('context', 'experts'))
- attn_gain_grad: float32 [2048], P('dp')
- query_proj_grad: float32 [2048, 3072], P('dp', 'experts')
- latent_proj_grad: float32 [2048, 576], P('dp')
- latent_gain_grad: float32 [512], P('dp')
- expand_proj_grad: float32 [512, 4096], P('dp', 'experts')
- output_proj_grad: float32 [2048, 2048], P('experts', 'dp')
- moe_gain_grad: float32 [2048], P('dp')
- router_proj_grad: float32 [2048, 16], P('dp')
- shared_in_grad: float32 [2048, 2, 2816], P('dp', None, 'experts')
- shared_out_grad: float32 [2816, 2048], P('experts', 'dp')
- expert_in_grad: float32 [16, 2048, 2, 1408], P(('context', 'experts'), None, None, 'dp')
- expert_out_grad: float32 [16, 1408, 2048], P(('context', 'experts'), 'dp')
The draws below stay inside these ranges and needn't reach their ends.
Inputs may be any that keep to these rules, and one draw needn't show every extreme that they name: `routes`: each token names 6 different experts; among the 128 tokens of one device no expert is named more than 64 times. `span_order`: A permutation: each position block appears once.
All inputs are finite; a program needn't handle non-finite values.
Results may differ from the reference program's by a relative error of at most 0.025.
Values may be sent and summed in bfloat16 or wider, within the bound.
A program may use at most 320 MiB of HBM per device.

```python
import math
from functools import partial
import jax
import jax.numpy as jnp
import numpy as np
from jax import lax

D = 2048
H = 16
NOPE = 128
ROPE = 64
VDIM = 128
RANK = 512
FF = 1408
SHARED = 2816
TOPK = 6
ROWS = 128
EXPERTS = 16
SEQS = 2
SEQ_LEN = 2048
HALF = 256
BLOCKS = 8
CAP = 64
N_DP = 2
N_CONTEXT = 4
N_EXPERTS = 4


def steps_of(own_key, dims, cuts, least, top_value):
    def one(position, blocks):
        heights = jax.random.uniform(jax.random.fold_in(jax.random.fold_in(own_key, 6), position), (blocks,), jnp.float32, least / len(cuts), top_value / len(cuts))
        return jnp.repeat(jnp.exp(heights), dims[position] // blocks).reshape((-1,) + (1,) * (len(dims) - position - 1))

    level = one(*cuts[0])
    for cut in cuts[1:]:
        level = level * one(*cut)
    return level


def deal_out(rng, own, number, rows, number_of, top, limit, skew):
    ranking = jax.random.permutation(rng, number_of)
    packed, ordinary = shares(number_of, rows * top, limit, skew, True), shares(number_of, rows * top, limit, skew, False)
    places = jnp.arange(number_of)

    def named(sizes, turn):
        used = int((sizes > 0).sum())
        fixed = max(1, used // 4)
        moved = fixed + (places - fixed + turn * (used - fixed)) % max(1, number_of - fixed)
        return jnp.zeros((number_of,), jnp.int32).at[ranking[jnp.where(places < fixed, places, moved)]].set(jnp.asarray(sizes, jnp.int32))

    sizes = jnp.where(number % 4 == 0, named(packed, number // 4), named(ordinary, number - number // 4 - 1))
    mixed = jax.random.permutation(jax.random.fold_in(own, 3), number_of)
    donor, receiver = mixed[0:number_of // 2 * 2:2], mixed[1:number_of // 2 * 2:2]
    margin = jnp.minimum(sizes[donor] - 1, limit - sizes[receiver]) // 2
    margin = jnp.where((donor == ranking[0]) | (receiver == ranking[0]) | (sizes[receiver] == 0), 0, jnp.maximum(margin, 0))
    moved = jax.random.randint(jax.random.fold_in(own, 4), (number_of // 2,), 0, 1 << 20) % (margin + 1)
    sizes = sizes.at[donor].add(-moved).at[receiver].add(moved)
    items = jnp.searchsorted(jnp.cumsum(sizes), jnp.arange(rows * top), side="right").astype(jnp.int32)
    grid = items.reshape(top, rows).T
    grid = grid[jax.random.permutation(jax.random.fold_in(own, 1), rows)]
    turn = jax.random.randint(jax.random.fold_in(own, 2), (rows, 1), 0, top)
    return jnp.take_along_axis(grid, (jnp.arange(top)[None, :] + turn) % top, axis=1)


def shares(count, total, limit, skew, full):
    loads = [(1 << 20) // math.isqrt(standing ** skew) + 1 for standing in range(1, count + 1)]
    largest = limit if full else min(limit, max(-(-total // count), total * loads[0] // sum(loads)))
    least = 1 if total - largest >= count - 1 else 0
    holding, surplus = [largest] + [least] * (count - 1), total - largest - least * (count - 1)
    while surplus > 0:
        candidates = [i for i in range(1, count) if holding[i] < largest] or [i for i in range(1, count) if holding[i] < limit]
        whole, remaining = sum([loads[i] for i in candidates]), surplus
        for i in candidates:
            addition = min(limit - holding[i], max(1, remaining * loads[i] // whole), surplus)
            holding[i] = holding[i] + addition
            surplus = surplus - addition
    return np.array(holding)


def noise(stream_key, extent, scale, bound, cuts=(), kind=jnp.bfloat16):
    values = jax.random.normal(stream_key, extent, jnp.float32) * scale
    if len(cuts) > 0:
        values = steps_of(stream_key, extent, cuts, -0.22, 0.18) * values
    return jnp.clip(values, min=-bound, max=bound).astype(kind)


def setup_inputs(seed: int = 0) -> dict:
    streams_of = jax.random.split(jax.random.key(seed), 17)
    layer_input = noise(streams_of[0], (SEQS, SEQ_LEN, D), 1.0, 6.0, ((0, 2), (1, 16)))
    cotangent = noise(streams_of[1], (SEQS, SEQ_LEN, D), 1.0, 6.0, ((0, 2), (1, 16)))
    routes_keys = jax.random.split(jax.random.fold_in(streams_of[2], 1), SEQS * SEQ_LEN // ROWS)
    routes_turns = jax.random.permutation(jax.random.fold_in(streams_of[2], 3), SEQS * SEQ_LEN // ROWS)
    routes = jax.vmap(lambda own, number: deal_out(jax.random.fold_in(streams_of[2], 2), own, number, ROWS, EXPERTS, TOPK, CAP, 2))(routes_keys, routes_turns).reshape((SEQS, SEQ_LEN, TOPK))
    span_order = jax.random.permutation(streams_of[3], BLOCKS).astype(jnp.int32)
    attn_gain = jnp.clip(1.0 + 0.1 * jax.random.normal(streams_of[4], (D,), jnp.float32), 0.5, 1.5).astype(jnp.bfloat16)
    query_proj = noise(streams_of[5], (D, H * (NOPE + ROPE)), D ** -0.5, 0.125, ((0, 2), (1, 4)))
    latent_proj = noise(streams_of[6], (D, RANK + ROPE), D ** -0.5, 0.125, ((0, 2),))
    latent_gain = jnp.clip(1.0 + 0.1 * jax.random.normal(streams_of[7], (RANK,), jnp.float32), 0.5, 1.5).astype(jnp.bfloat16)
    expand_proj = noise(streams_of[8], (RANK, H * (NOPE + VDIM)), RANK ** -0.5, 0.25, ((0, 2), (1, 4)))
    output_proj = noise(streams_of[9], (H * VDIM, D), (H * VDIM // 8) ** -0.5, 0.375, ((0, 4), (1, 2)))
    moe_gain = jnp.clip(1.0 + 0.1 * jax.random.normal(streams_of[10], (D,), jnp.float32), 0.5, 1.5).astype(jnp.bfloat16)
    router_proj = noise(streams_of[11], (D, EXPERTS), (D // 4) ** -0.5, 0.25, ((0, 2),))
    shared_in = noise(streams_of[12], (D, 2, SHARED), D ** -0.5, 0.125, ((0, 2), (2, 4)))
    shared_out = noise(streams_of[13], (SHARED, D), SHARED ** -0.5, 0.109375, ((0, 4), (1, 2)))
    expert_in = noise(streams_of[14], (EXPERTS, D, 2, FF), D ** -0.5, 0.125, ((0, 16), (3, 2)))
    expert_out = noise(streams_of[15], (EXPERTS, FF, D), FF ** -0.5, 0.15625, ((0, 16), (1, 2)))
    return dict(layer_input=layer_input, cotangent=cotangent, routes=routes, span_order=span_order, attn_gain=attn_gain, query_proj=query_proj, latent_proj=latent_proj, latent_gain=latent_gain, expand_proj=expand_proj, output_proj=output_proj, moe_gain=moe_gain, router_proj=router_proj, shared_in=shared_in, shared_out=shared_out, expert_in=expert_in, expert_out=expert_out)


eps_norm = 1e-06
route_scale = 2.446
rope_base = 50000.0
masked_value = -1e+30

def round_bf(values):
    return lax.optimization_barrier(values.astype(jnp.bfloat16)).astype(jnp.float32)

def rope_tables(positions, width):
    count = width // 2
    exponents = jnp.arange(count, dtype=jnp.float32) * (2.0 / width)
    freqs = jnp.power(jnp.float32(rope_base), -exponents)
    angles = positions.astype(jnp.float32)[:, None] * freqs[None, :]
    cosine = jnp.cos(angles)
    sine = jnp.sin(angles)
    return (jnp.concatenate([cosine, cosine], axis=1), jnp.concatenate([sine, sine], axis=1))

def rotate(values, cosine, sine):
    count = values.shape[-1] // 2
    turned = jnp.concatenate([-values[..., count:], values[..., :count]], axis=-1)
    return values * cosine + turned * sine

def rotate_back(grads, cosine, sine):
    count = grads.shape[-1] // 2
    scaled = grads * sine
    turned = jnp.concatenate([scaled[..., count:], -scaled[..., :count]], axis=-1)
    return grads * cosine + turned

def rms_back(grad_normed, values, scale, gain):
    gained = grad_normed * gain
    gain_grad = lax.optimization_barrier(jnp.sum(grad_normed * values * scale, axis=0))
    value_grad = scale * gained - values * (scale * scale * scale) * lax.optimization_barrier(jnp.mean(gained * values, axis=1, keepdims=True))
    return (value_grad, gain_grad)

def gated_act(pre, width):
    gate = pre[:, :width]
    return (gate * jax.nn.sigmoid(gate) * pre[:, width:]).astype(jnp.bfloat16)

def gated_back(act_grad, pre, width):
    gate = pre[:, :width]
    upper = pre[:, width:]
    sig = jax.nn.sigmoid(gate)
    return jnp.concatenate([act_grad * upper * sig * (1.0 + gate * (1.0 - sig)), act_grad * gate * sig], axis=1).astype(jnp.bfloat16)

def expert_forward(rows, gate_up, down):
    width = down.shape[0]
    pre = jnp.dot(rows, gate_up.reshape(gate_up.shape[0], 2 * width), preferred_element_type=jnp.float32)
    result = jnp.dot(gated_act(pre, width), down, preferred_element_type=jnp.float32).astype(jnp.bfloat16)
    return (result, pre)

def expert_backward(rows, pre, grad_rows, gate_up, down):
    width = down.shape[0]
    flat = gate_up.reshape(gate_up.shape[0], 2 * width)
    act_grad = jnp.dot(grad_rows, down.T, preferred_element_type=jnp.float32)
    pre_grad = gated_back(act_grad, pre, width)
    down_grad = jnp.dot(gated_act(pre, width).T, grad_rows, preferred_element_type=jnp.float32)
    in_grad = jnp.dot(rows.T, pre_grad, preferred_element_type=jnp.float32).reshape(gate_up.shape)
    back = jnp.dot(pre_grad, flat.T, preferred_element_type=jnp.float32).astype(jnp.bfloat16)
    return (back, in_grad, down_grad)

def expert_pass(rows, gate_up, down):
    width = FF // N_DP
    total = jnp.zeros((rows.shape[0], D), jnp.float32)
    for part in range(N_DP):
        result, unused = expert_forward(rows, gate_up[:, :, part * width:(part + 1) * width], down[part * width:(part + 1) * width])
        total = total + result.astype(jnp.float32)
    return total

def expert_grads(rows, grad_rows, gate_up, down):
    width = FF // N_DP
    total = jnp.zeros((rows.shape[0], D), jnp.float32)
    in_parts = []
    down_parts = []
    for part in range(N_DP):
        piece_in = gate_up[:, :, part * width:(part + 1) * width]
        piece_down = down[part * width:(part + 1) * width]
        unused, pre = expert_forward(rows, piece_in, piece_down)
        back, in_grad, down_grad = expert_backward(rows, pre, grad_rows, piece_in, piece_down)
        total = total + back.astype(jnp.float32)
        in_parts.append(in_grad)
        down_parts.append(down_grad)
    return (total, jnp.concatenate(in_parts, axis=2), jnp.concatenate(down_parts, axis=0))

def slot_places(route_block, experts, capacity):
    flat = route_block.reshape(-1)
    hits = (flat[:, None] == jnp.arange(experts, dtype=jnp.int32)[None, :]).astype(jnp.int32)
    ranks = lax.optimization_barrier(jnp.sum(hits * jnp.cumsum(hits, axis=0), axis=1)) - 1
    return (flat * capacity + ranks).astype(jnp.int32)

def masked_scores(query_block, query_pos, keys, rope_keys, key_pos, score_scale):
    scores = jnp.einsum('qhd,khd->hqk', query_block[:, :, :NOPE], keys[:, :, :NOPE])
    scores = scores + jnp.einsum('qhd,kd->hqk', query_block[:, :, NOPE:], rope_keys)
    scores = scores * score_scale
    allowed = key_pos[None, :] <= query_pos[:, None]
    return jnp.where(allowed[None, :, :], scores, masked_value)

def attend_forward(queries, keyvals, rope_keys, positions):
    score_scale = 1.0 / math.sqrt(NOPE + ROPE)
    key_float = keyvals.astype(jnp.float32)
    rope_float = rope_keys.astype(jnp.float32)

    def step(carry, block):
        start = block * HALF
        query_block = lax.dynamic_slice_in_dim(queries, start, HALF, 0).astype(jnp.float32)
        query_pos = lax.dynamic_slice_in_dim(positions, start, HALF, 0)
        scores = masked_scores(query_block, query_pos, key_float, rope_float, positions, score_scale)
        top = lax.optimization_barrier(jnp.max(scores, axis=2, keepdims=True))
        lse = top[:, :, 0] + jnp.log(lax.optimization_barrier(jnp.sum(jnp.exp(scores - top), axis=2)))
        probs = round_bf(jnp.exp(scores - lse[:, :, None]))
        result = jnp.einsum('hqk,khd->qhd', probs, key_float[:, :, NOPE:]).astype(jnp.bfloat16)
        return (carry, (result, lse))
    unused, (results, lses) = lax.scan(step, jnp.int32(0), jnp.arange(BLOCKS, dtype=jnp.int32))
    return (results.reshape(SEQ_LEN, H, VDIM), lses.transpose(1, 0, 2).reshape(H, SEQ_LEN))

def attend_backward(queries, keyvals, rope_keys, attended, lse, attended_grad, positions):
    score_scale = 1.0 / math.sqrt(NOPE + ROPE)
    key_float = keyvals.astype(jnp.float32)
    rope_float = rope_keys.astype(jnp.float32)

    def step(carry, block):
        keyval_grad, rope_grad = carry
        start = block * HALF
        query_block = lax.dynamic_slice_in_dim(queries, start, HALF, 0).astype(jnp.float32)
        out_block = lax.dynamic_slice_in_dim(attended, start, HALF, 0).astype(jnp.float32)
        grad_block = lax.dynamic_slice_in_dim(attended_grad, start, HALF, 0).astype(jnp.float32)
        query_pos = lax.dynamic_slice_in_dim(positions, start, HALF, 0)
        scores = masked_scores(query_block, query_pos, key_float, rope_float, positions, score_scale)
        probs = jnp.exp(scores - lax.dynamic_slice_in_dim(lse, start, HALF, 1)[:, :, None])
        prob_round = round_bf(probs)
        prob_grad = jnp.einsum('qhd,khd->hqk', grad_block, key_float[:, :, NOPE:])
        delta = lax.optimization_barrier(jnp.sum(out_block * grad_block, axis=2)).T
        score_grad = round_bf(probs * (prob_grad - delta[:, :, None]))
        query_grad = score_scale * jnp.concatenate([jnp.einsum('hqk,khd->qhd', score_grad, key_float[:, :, :NOPE]), jnp.einsum('hqk,kd->qhd', score_grad, rope_float)], axis=2)
        keyval_grad = keyval_grad + jnp.concatenate([score_scale * jnp.einsum('hqk,qhd->khd', score_grad, query_block[:, :, :NOPE]), jnp.einsum('hqk,qhd->khd', prob_round, grad_block)], axis=2)
        rope_grad = rope_grad + score_scale * jnp.einsum('hqk,qhd->kd', score_grad, query_block[:, :, NOPE:])
        return ((keyval_grad, rope_grad), query_grad)
    start_grads = (jnp.zeros((SEQ_LEN, H, NOPE + VDIM), jnp.float32), jnp.zeros((SEQ_LEN, ROPE), jnp.float32))
    (keyval_grad, rope_grad), query_grads = lax.scan(step, start_grads, jnp.arange(BLOCKS, dtype=jnp.int32))
    return (query_grads.reshape(SEQ_LEN, H, NOPE + ROPE), keyval_grad, rope_grad)

def reference(layer_input, cotangent, routes, span_order, attn_gain, query_proj, latent_proj, latent_gain, expand_proj, output_proj, moe_gain, router_proj, shared_in, shared_out, expert_in, expert_out):
    tokens = SEQS * SEQ_LEN
    sources = SEQS * N_CONTEXT * N_EXPERTS
    rows = jnp.arange(SEQ_LEN, dtype=jnp.int32)
    positions = (span_order[rows // HALF] * HALF + rows % HALF).astype(jnp.int32)
    cosine, sine = rope_tables(positions, ROPE)
    cos_all = jnp.tile(cosine, (SEQS, 1))
    sin_all = jnp.tile(sine, (SEQS, 1))
    inputs = layer_input.reshape(tokens, D).astype(jnp.float32)
    scale_one = lax.rsqrt(lax.optimization_barrier(jnp.mean(inputs * inputs, axis=1, keepdims=True)) + eps_norm)
    normed = (inputs * scale_one * attn_gain.astype(jnp.float32)).astype(jnp.bfloat16)
    query_raw = jnp.dot(normed, query_proj, preferred_element_type=jnp.float32).reshape(tokens, H, NOPE + ROPE)
    queries = jnp.concatenate([query_raw[:, :, :NOPE], rotate(query_raw[:, :, NOPE:], cos_all[:, None, :], sin_all[:, None, :])], axis=2).astype(jnp.bfloat16)
    compressed = jnp.dot(normed, latent_proj, preferred_element_type=jnp.float32)
    latent = compressed[:, :RANK]
    scale_latent = lax.rsqrt(lax.optimization_barrier(jnp.mean(latent * latent, axis=1, keepdims=True)) + eps_norm)
    latent_normed = (latent * scale_latent * latent_gain.astype(jnp.float32)).astype(jnp.bfloat16)
    rope_keys = rotate(compressed[:, RANK:], cos_all, sin_all).astype(jnp.bfloat16)
    keyvals = jnp.dot(latent_normed, expand_proj, preferred_element_type=jnp.float32).astype(jnp.bfloat16).reshape(tokens, H, NOPE + VDIM)

    def forward_one(pieces):
        return attend_forward(pieces[0], pieces[1], pieces[2], positions)
    seq_queries = queries.reshape(SEQS, SEQ_LEN, H, NOPE + ROPE)
    seq_keyvals = keyvals.reshape(SEQS, SEQ_LEN, H, NOPE + VDIM)
    seq_rope = rope_keys.reshape(SEQS, SEQ_LEN, ROPE)
    attended_seq, lse_seq = lax.map(forward_one, (seq_queries, seq_keyvals, seq_rope))
    attended = attended_seq.reshape(tokens, H * VDIM)
    hidden = inputs + jnp.dot(attended, output_proj, preferred_element_type=jnp.float32)
    scale_two = lax.rsqrt(lax.optimization_barrier(jnp.mean(hidden * hidden, axis=1, keepdims=True)) + eps_norm)
    hidden_normed = (hidden * scale_two * moe_gain.astype(jnp.float32)).astype(jnp.bfloat16)
    gates = jax.nn.sigmoid(jnp.dot(hidden_normed, router_proj, preferred_element_type=jnp.float32))
    route_rows = routes.reshape(tokens, TOPK)
    picked = (route_rows[:, :, None] == jnp.arange(EXPERTS, dtype=jnp.int32)[None, None, :]).astype(jnp.float32)
    chosen = lax.optimization_barrier(jnp.sum(picked * gates[:, None, :], axis=2))
    chosen_total = lax.optimization_barrier(jnp.sum(chosen, axis=1, keepdims=True))
    route_weights = route_scale * chosen / chosen_total
    places = jax.vmap(partial(slot_places, experts=EXPERTS, capacity=CAP))(route_rows.reshape(sources, ROWS, TOPK))

    def fill_one(place, block_rows):
        return jnp.zeros((EXPERTS * CAP, D), jnp.bfloat16).at[place].set(block_rows)

    def fill(values):
        buffers = jax.vmap(fill_one)(places, values.reshape(sources, ROWS * TOPK, D))
        return buffers.reshape(sources, EXPERTS, CAP, D).transpose(1, 0, 2, 3).reshape(EXPERTS, sources * CAP, D)

    def take_one(block_buffer, place):
        return block_buffer[place]

    def unfill(buffers):
        flat = buffers.reshape(EXPERTS, sources, CAP, D).transpose(1, 0, 2, 3).reshape(sources, EXPERTS * CAP, D)
        return jax.vmap(take_one)(flat, places).reshape(tokens, TOPK, D)
    arriving = fill(jnp.repeat(hidden_normed, TOPK, axis=0))

    def forward_expert(pieces):
        return expert_pass(pieces[0], pieces[1], pieces[2])
    expert_rows = unfill(lax.map(forward_expert, (arriving, expert_in, expert_out)))
    routed = lax.optimization_barrier(jnp.sum(route_weights[:, :, None] * expert_rows, axis=1))
    shared_flat = shared_in.reshape(D, 2 * SHARED)
    shared_pre = jnp.dot(hidden_normed, shared_flat, preferred_element_type=jnp.float32)
    shared_act = gated_act(shared_pre, SHARED)
    block_output = hidden + routed + jnp.dot(shared_act, shared_out, preferred_element_type=jnp.float32)
    cot = cotangent.reshape(tokens, D)
    cot_float = cot.astype(jnp.float32)
    shared_pre_grad = gated_back(jnp.dot(cot, shared_out.T, preferred_element_type=jnp.float32), shared_pre, SHARED)
    shared_out_grad = jnp.dot(shared_act.T, cot, preferred_element_type=jnp.float32)
    shared_in_grad = jnp.dot(hidden_normed.T, shared_pre_grad, preferred_element_type=jnp.float32).reshape(D, 2, SHARED)
    normed_grad = jnp.dot(shared_pre_grad, shared_flat.T, preferred_element_type=jnp.float32)
    weight_grad = lax.optimization_barrier(jnp.sum(cot_float[:, None, :] * expert_rows, axis=2))
    sent = (route_weights[:, :, None] * cot_float[:, None, :]).astype(jnp.bfloat16)
    arriving_grad = fill(sent.reshape(tokens * TOPK, D))

    def backward_expert(pieces):
        return expert_grads(pieces[0], pieces[1], pieces[2], pieces[3])
    backs, expert_in_grad, expert_out_grad = lax.map(backward_expert, (arriving, arriving_grad, expert_in, expert_out))
    routed_grad = lax.optimization_barrier(jnp.sum(unfill(backs), axis=1))
    chosen_grad = route_scale * weight_grad / chosen_total - route_scale * lax.optimization_barrier(jnp.sum(weight_grad * chosen, axis=1, keepdims=True)) / (chosen_total * chosen_total)
    logit_grad = lax.optimization_barrier(jnp.sum(picked * (chosen_grad * chosen * (1.0 - chosen))[:, :, None], axis=1))
    normed_grad = normed_grad + routed_grad + jnp.dot(logit_grad, router_proj.astype(jnp.float32).T, precision=lax.Precision.HIGHEST)
    router_grad = jnp.dot(hidden_normed.astype(jnp.float32).T, logit_grad, precision=lax.Precision.HIGHEST)
    norm_part, moe_gain_grad = rms_back(normed_grad, hidden, scale_two, moe_gain.astype(jnp.float32))
    hidden_grad = cot_float + norm_part
    hidden_round = hidden_grad.astype(jnp.bfloat16)
    output_proj_grad = jnp.dot(attended.T, hidden_round, preferred_element_type=jnp.float32)
    attended_grad = jnp.dot(hidden_round, output_proj.T, preferred_element_type=jnp.float32).astype(jnp.bfloat16)

    def backward_one(pieces):
        return attend_backward(pieces[0], pieces[1], pieces[2], pieces[3], pieces[4], pieces[5], positions)
    query_grad, keyval_grad, rope_grad = lax.map(backward_one, (seq_queries, seq_keyvals, seq_rope, attended_seq, lse_seq, attended_grad.reshape(SEQS, SEQ_LEN, H, VDIM)))
    query_grad = query_grad.reshape(tokens, H, NOPE + ROPE)
    query_raw_grad = jnp.concatenate([query_grad[:, :, :NOPE], rotate_back(query_grad[:, :, NOPE:], cos_all[:, None, :], sin_all[:, None, :])], axis=2).reshape(tokens, H * (NOPE + ROPE)).astype(jnp.bfloat16)
    query_proj_grad = jnp.dot(normed.T, query_raw_grad, preferred_element_type=jnp.float32)
    keyval_flat = keyval_grad.reshape(tokens, H * (NOPE + VDIM))
    latent_normed_grad = jnp.dot(keyval_flat, expand_proj.astype(jnp.float32).T, precision=lax.Precision.HIGHEST)
    expand_proj_grad = jnp.dot(latent_normed.astype(jnp.float32).T, keyval_flat, precision=lax.Precision.HIGHEST)
    latent_grad, latent_gain_grad = rms_back(latent_normed_grad, latent, scale_latent, latent_gain.astype(jnp.float32))
    compressed_grad = jnp.concatenate([latent_grad, rotate_back(rope_grad.reshape(tokens, ROPE), cos_all, sin_all)], axis=1).astype(jnp.bfloat16)
    latent_proj_grad = jnp.dot(normed.T, compressed_grad, preferred_element_type=jnp.float32)
    input_normed_grad = jnp.dot(query_raw_grad, query_proj.T, preferred_element_type=jnp.float32) + jnp.dot(compressed_grad, latent_proj.T, preferred_element_type=jnp.float32)
    first_part, attn_gain_grad = rms_back(input_normed_grad, inputs, scale_one, attn_gain.astype(jnp.float32))
    input_grad = hidden_grad + first_part
    return (block_output.reshape(SEQS, SEQ_LEN, D), input_grad.reshape(SEQS, SEQ_LEN, D), attn_gain_grad, query_proj_grad, latent_proj_grad, latent_gain_grad, expand_proj_grad, output_proj_grad, moe_gain_grad, router_grad, shared_in_grad, shared_out_grad, expert_in_grad, expert_out_grad)
```

```python
import math

import jax
import jax.numpy as jnp
from jax import lax
from jax.experimental import pallas as pl
from jax.experimental.pallas import tpu as pltpu
from jax.sharding import PartitionSpec as P


D = 2048
NOPE = 128
ROPE = 64
VDIM = 128
RANK = 512
TOPK = 6


eps_norm = 1e-06
route_scale = 2.446
rope_base = 50000.0
masked_value = -1e30


def rope_tables(positions, width):
    count = width // 2
    exponents = jnp.arange(count, dtype=jnp.float32) * (2.0 / width)
    freqs = jnp.power(jnp.float32(rope_base), -exponents)
    angles = positions.astype(jnp.float32)[:, None] * freqs[None, :]
    cosine = jnp.cos(angles)
    sine = jnp.sin(angles)
    return (jnp.concatenate([cosine, cosine], axis=1), jnp.concatenate([sine, sine], axis=1))


def rotate(values, cosine, sine):
    count = values.shape[-1] // 2
    turned = jnp.concatenate([-values[..., count:], values[..., :count]], axis=-1)
    return values * cosine + turned * sine


def rotate_back(grads, cosine, sine):
    count = grads.shape[-1] // 2
    scaled = grads * sine
    turned = jnp.concatenate([scaled[..., count:], -scaled[..., :count]], axis=-1)
    return grads * cosine + turned


def rms_back(grad_normed, values, scale, gain):
    gained = grad_normed * gain
    gain_grad = jnp.sum(grad_normed * values * scale, axis=0)
    value_grad = scale * gained - values * (scale * scale * scale) * jnp.mean(
        gained * values, axis=1, keepdims=True
    )
    return (value_grad, gain_grad)


EVERY = ("dp", "context", "experts")
NT = (((1,), (1,)), ((), ()))
TN = (((0,), (0,)), ((), ()))


def mm(left, right, dims=None):
    if dims is None:
        return jnp.dot(left, right, preferred_element_type=jnp.float32)
    return lax.dot_general(left, right, dims, preferred_element_type=jnp.float32)


def gate(*values):
    return lax.optimization_barrier(values)


def swap(values, axis, mask):
    count = lax.axis_size(axis)
    return lax.ppermute(values, axis, [(i, i ^ mask) for i in range(count)])


def masks_of(axis):
    count = lax.axis_size(axis)
    return [1 << bit for bit in range(count.bit_length() - 1)]


def cube_gather(values, axis):
    held = {0: values}
    for mask in reversed(masks_of(axis)):
        keys = sorted(held)
        rows = values.shape[0]
        got = swap(jnp.concatenate([held[key] for key in keys], axis=0), axis, mask)
        for at, key in enumerate(keys):
            held[key | mask] = got[at * rows : (at + 1) * rows]
    return jnp.concatenate([held[key] for key in sorted(held)], axis=0)


def cube_scatter(values, axis):
    count = lax.axis_size(axis)
    rows = values.shape[0] // count
    held = {key: values[key * rows : (key + 1) * rows] for key in range(count)}
    for mask in masks_of(axis):
        kept = [key for key in sorted(held) if not key & mask]
        sent = jnp.concatenate([held[key | mask] for key in kept], axis=0)
        got = swap(sent.astype(jnp.bfloat16), axis, mask).astype(jnp.float32)
        held = {
            key: held[key].astype(jnp.float32) + got[at * rows : (at + 1) * rows]
            for at, key in enumerate(kept)
        }
    return held[0]


def sum_everywhere(values):
    for axis in ("experts", "context", "dp"):
        for mask in masks_of(axis):
            values = values + swap(values, axis, mask)
    return values


def join_dp(values, other, axis):
    first = lax.axis_index("dp") == 0
    return jnp.where(
        first,
        jnp.concatenate([values, other], axis=axis),
        jnp.concatenate([other, values], axis=axis),
    )


def pick_rows(take, parts, width):
    sources, capacity, rows_dev = take.shape
    per = 4
    wide = [part.shape[1] for part in parts]

    def body(take_ref, *refs):
        out_ref = refs[-1]
        for one in range(per):
            start = 0
            for ref in refs[:-1]:
                span = min(ref.shape[1], width - start)
                out_ref[one * capacity : (one + 1) * capacity, start : start + span] = mm(
                    take_ref[one], ref[one * rows_dev : (one + 1) * rows_dev, :span]
                ).astype(jnp.bfloat16)
                start += span

    return pl.pallas_call(
        body,
        grid=(sources // per,),
        in_specs=[pl.BlockSpec((per, capacity, rows_dev), lambda s: (s, 0, 0))]
        + [pl.BlockSpec((per * rows_dev, size), lambda s: (s, 0)) for size in wide],
        out_specs=pl.BlockSpec((per * capacity, width), lambda s: (s, 0)),
        out_shape=jax.ShapeDtypeStruct((sources * capacity, width), jnp.bfloat16),
        compiler_params=pltpu.CompilerParams(vmem_limit_bytes=40 << 20),
        cost_estimate=pl.CostEstimate(
            flops=2 * sources * capacity * rows_dev * width,
            bytes_accessed=2 * sources * (rows_dev + capacity) * width,
            transcendentals=0,
        ),
        name="pick_rows",
    )(take, *parts)


def place_rows(take, values, extra, widths):
    sources, capacity, rows_dev = take.shape
    per = 4
    inputs = [values] if extra is None else [values, extra]
    shapes = list(widths)
    if extra is not None:
        shapes[-1] += extra.shape[1]

    def body(take_ref, *refs):
        ins, outs = refs[: len(inputs)], refs[len(inputs) :]
        for one in range(per):
            slots = slice(one * capacity, (one + 1) * capacity)
            rows = slice(one * rows_dev, (one + 1) * rows_dev)
            start = 0
            for ref, span in zip(outs, widths):
                ref[rows, :span] = mm(
                    take_ref[one], ins[0][slots, start : start + span], TN
                ).astype(jnp.bfloat16)
                start += span
            if extra is not None:
                outs[-1][rows, widths[-1] :] = mm(take_ref[one], ins[1][slots, :], TN).astype(
                    jnp.bfloat16
                )

    return pl.pallas_call(
        body,
        grid=(sources // per,),
        in_specs=[pl.BlockSpec((per, capacity, rows_dev), lambda s: (s, 0, 0))]
        + [pl.BlockSpec((per * capacity, one.shape[1]), lambda s: (s, 0)) for one in inputs],
        out_specs=[pl.BlockSpec((per * rows_dev, size), lambda s: (s, 0)) for size in shapes],
        out_shape=[
            jax.ShapeDtypeStruct((sources * rows_dev, size), jnp.bfloat16) for size in shapes
        ],
        compiler_params=pltpu.CompilerParams(vmem_limit_bytes=40 << 20),
        cost_estimate=pl.CostEstimate(
            flops=2 * sources * capacity * rows_dev * sum(shapes),
            bytes_accessed=2 * sources * (rows_dev + capacity) * sum(shapes),
            transcendentals=0,
        ),
        name="place_rows",
    )(take, *inputs)


def gated_parts(gate, upper, act_grad):
    sig = jax.nn.sigmoid(gate)
    act = (gate * sig * upper).astype(jnp.bfloat16)
    pre_grad = jnp.concatenate(
        [act_grad * upper * sig * (1.0 + gate * (1.0 - sig)), act_grad * gate * sig], axis=1
    ).astype(jnp.bfloat16)
    return act, pre_grad


def attend_fwd_body(scale, qn_ref, qr_ref, kv_ref, kr_ref, qp_ref, kp_ref, out_ref, lse_ref):
    scores = mm(qn_ref[...], kv_ref[:, :NOPE], NT) + mm(qr_ref[0], kr_ref[...], NT)
    scores = jnp.where(kp_ref[...] <= qp_ref[...], scores * scale, masked_value)
    top = jnp.max(scores, axis=1, keepdims=True)
    weights = jnp.exp(scores - top)
    total = jnp.sum(weights, axis=1, keepdims=True)
    out = mm(weights.astype(jnp.bfloat16), kv_ref[:, NOPE:])
    out_ref[...] = (out / total).astype(jnp.bfloat16)
    lse_ref[0] = top + jnp.log(total)


def attend_fwd(q_nope, q_rope, keyvals, rope_keys, q_pos, k_pos, scale):
    heads, rows, rope = q_rope.shape
    keys = keyvals.shape[0]
    tile = min(rows, 256)
    return pl.pallas_call(
        lambda *refs: attend_fwd_body(scale, *refs),
        grid=(heads, rows // tile),
        in_specs=[
            pl.BlockSpec((tile, NOPE), lambda h, i: (i, h)),
            pl.BlockSpec((1, tile, rope), lambda h, i: (h, i, 0)),
            pl.BlockSpec((keys, NOPE + VDIM), lambda h, i: (0, h)),
            pl.BlockSpec((keys, rope), lambda h, i: (0, 0)),
            pl.BlockSpec((tile, 1), lambda h, i: (i, 0)),
            pl.BlockSpec((1, keys), lambda h, i: (0, 0)),
        ],
        out_specs=[
            pl.BlockSpec((tile, VDIM), lambda h, i: (i, h)),
            pl.BlockSpec((1, tile, 1), lambda h, i: (h, i, 0)),
        ],
        out_shape=[
            jax.ShapeDtypeStruct((rows, heads * VDIM), jnp.bfloat16),
            jax.ShapeDtypeStruct((heads, rows, 1), jnp.float32),
        ],
        compiler_params=pltpu.CompilerParams(vmem_limit_bytes=60 << 20),
        cost_estimate=pl.CostEstimate(
            flops=2 * heads * rows * keys * (NOPE + rope + VDIM),
            bytes_accessed=4 * keys * heads * (NOPE + VDIM),
            transcendentals=heads * rows * keys,
        ),
        name="attend_fwd",
    )(q_nope, q_rope, keyvals, rope_keys, q_pos, k_pos)


def attend_bwd_body(
    scale,
    qn_ref,
    qr_ref,
    kv_ref,
    kr_ref,
    qp_ref,
    kp_ref,
    out_ref,
    grad_ref,
    lse_ref,
    dqn_ref,
    dqr_ref,
    dkv_ref,
    dkr_ref,
    dk_sum,
    dv_sum,
    dr_sum,
):
    head, tile = pl.program_id(1), pl.program_id(2)
    tiles = pl.num_programs(2)
    grad = grad_ref[...]
    q_nope, q_rope = qn_ref[...], qr_ref[0]
    keys, values = kv_ref[:, :NOPE], kv_ref[:, NOPE:]
    scores = mm(q_nope, keys, NT) + mm(q_rope, kr_ref[...], NT)
    probs = jnp.exp(scores * scale - lse_ref[0])
    probs = jnp.where(kp_ref[...] <= qp_ref[...], probs, 0.0)
    delta = jnp.sum(
        out_ref[...].astype(jnp.float32) * grad.astype(jnp.float32), axis=1, keepdims=True
    )
    score_grad = (probs * (mm(grad, values, NT) - delta)).astype(jnp.bfloat16)
    dqn_ref[0] = scale * mm(score_grad, keys)
    dqr_ref[0, 0] = scale * mm(score_grad, kr_ref[...])
    key_part = mm(score_grad, q_nope, TN)
    value_part = mm(probs.astype(jnp.bfloat16), grad, TN)
    rope_part = mm(score_grad, q_rope, TN)

    @pl.when(tile == 0)
    def _():
        dk_sum[...] = key_part
        dv_sum[...] = value_part

    @pl.when(tile > 0)
    def _():
        dk_sum[...] += key_part
        dv_sum[...] += value_part

    @pl.when((tile == 0) & (head == 0))
    def _():
        dr_sum[...] = rope_part

    @pl.when((tile > 0) | (head > 0))
    def _():
        dr_sum[...] += rope_part

    @pl.when(tile == tiles - 1)
    def _():
        dkv_ref[:, :NOPE] = (scale * dk_sum[...]).astype(jnp.bfloat16)
        dkv_ref[:, NOPE:] = dv_sum[...].astype(jnp.bfloat16)

    @pl.when((tile == tiles - 1) & (head == pl.num_programs(1) - 1))
    def _():
        dkr_ref[...] = (scale * dr_sum[...]).astype(jnp.bfloat16)


def attend_bwd(q_nope, q_rope, keyvals, rope_keys, q_pos, k_pos, attended, grad, lse, scale):
    heads, rows, rope = q_rope.shape
    keys = keyvals.shape[0]
    tile = min(rows, 256)
    chunk = min(keys, 2048)
    chunks = keys // chunk
    dqn, dqr, dkv, dkr = pl.pallas_call(
        lambda *refs: attend_bwd_body(scale, *refs),
        grid=(chunks, heads, rows // tile),
        in_specs=[
            pl.BlockSpec((tile, NOPE), lambda c, h, i: (i, h)),
            pl.BlockSpec((1, tile, rope), lambda c, h, i: (h, i, 0)),
            pl.BlockSpec((chunk, NOPE + VDIM), lambda c, h, i: (c, h)),
            pl.BlockSpec((chunk, rope), lambda c, h, i: (c, 0)),
            pl.BlockSpec((tile, 1), lambda c, h, i: (i, 0)),
            pl.BlockSpec((1, chunk), lambda c, h, i: (0, c)),
            pl.BlockSpec((tile, VDIM), lambda c, h, i: (i, h)),
            pl.BlockSpec((tile, VDIM), lambda c, h, i: (i, h)),
            pl.BlockSpec((1, tile, 1), lambda c, h, i: (h, i, 0)),
        ],
        out_specs=[
            pl.BlockSpec((1, tile, NOPE), lambda c, h, i: (c, i, h)),
            pl.BlockSpec((1, 1, tile, rope), lambda c, h, i: (c, h, i, 0)),
            pl.BlockSpec((chunk, NOPE + VDIM), lambda c, h, i: (c, h)),
            pl.BlockSpec((chunk, rope), lambda c, h, i: (c, 0)),
        ],
        out_shape=[
            jax.ShapeDtypeStruct((chunks, rows, heads * NOPE), jnp.float32),
            jax.ShapeDtypeStruct((chunks, heads, rows, rope), jnp.float32),
            jax.ShapeDtypeStruct((keys, heads * (NOPE + VDIM)), jnp.bfloat16),
            jax.ShapeDtypeStruct((keys, rope), jnp.bfloat16),
        ],
        scratch_shapes=[
            pltpu.VMEM((chunk, NOPE), jnp.float32),
            pltpu.VMEM((chunk, VDIM), jnp.float32),
            pltpu.VMEM((chunk, rope), jnp.float32),
        ],
        compiler_params=pltpu.CompilerParams(vmem_limit_bytes=60 << 20),
        cost_estimate=pl.CostEstimate(
            flops=2 * heads * rows * keys * (3 * NOPE + 3 * rope + 2 * VDIM),
            bytes_accessed=8 * keys * heads * (NOPE + VDIM),
            transcendentals=heads * rows * keys,
        ),
        name="attend_bwd",
    )(q_nope, q_rope, keyvals, rope_keys, q_pos, k_pos, attended, grad, lse)
    return jnp.sum(dqn, axis=0), jnp.sum(dqr, axis=0), dkv, dkr


def layer(
    layer_input,
    cotangent,
    routes,
    span_order,
    attn_gain,
    query_proj,
    latent_proj,
    latent_gain,
    expand_proj,
    output_proj,
    moe_gain,
    router_proj,
    shared_in,
    shared_out,
    expert_in,
    expert_out,
):
    place_dp = lax.axis_index("dp")
    place_context = lax.axis_index("context")
    place_experts = lax.axis_index("experts")
    count_dp = lax.axis_size("dp")
    count_context = lax.axis_size("context")
    count_experts = lax.axis_size("experts")
    own_in = layer_input[0]
    own_cot = cotangent[0]
    rows_dev = own_in.shape[0]
    sources = count_dp * count_context * count_experts
    heads = query_proj.shape[1] // (NOPE + ROPE)
    experts = router_proj.shape[1]
    shared_width = shared_out.shape[0]
    width = expert_out.shape[1]
    score_scale = 1.0 / math.sqrt(NOPE + ROPE)

    span_rows = count_experts * rows_dev
    total_rows = span_rows * count_context
    half = span_rows // 2
    width_dp = D // count_dp
    near = place_dp * width_dp
    far = (1 - place_dp) * width_dp

    names = jnp.arange(experts, dtype=jnp.int32)
    route_code = jnp.pad(routes[0], ((0, 0), (0, 128 - TOPK))).astype(jnp.bfloat16)
    all_routes = lax.all_gather(route_code, EVERY, axis=0, tiled=True)
    all_routes = all_routes[:, :TOPK].astype(jnp.int32)
    all_cot = lax.all_gather(own_cot, EVERY, axis=0, tiled=True)

    small = jnp.concatenate([attn_gain, latent_gain, moe_gain, router_proj.reshape(-1)])
    cuts = [attn_gain.size, latent_gain.size, moe_gain.size, router_proj.size]
    starts = [sum(cuts[:i]) for i in range(4)]
    small = join_dp(small[None], swap(small, "dp", 1)[None], 0)
    attn_gain, latent_gain, moe_gain, router_flat = (
        small[:, start : start + size].reshape(-1) for start, size in zip(starts, cuts)
    )
    router_proj = router_flat.reshape(-1, experts)
    attn_gain, latent_gain, moe_gain = (
        gain.astype(jnp.float32) for gain in (attn_gain, latent_gain, moe_gain)
    )

    inputs = own_in.astype(jnp.float32)
    scale_one = lax.rsqrt(jnp.mean(inputs * inputs, axis=1, keepdims=True) + eps_norm)
    own_normed = (inputs * scale_one * attn_gain).astype(jnp.bfloat16)
    latent_shard = latent_proj.T
    far_normed = swap(lax.dynamic_slice_in_dim(own_normed, far, width_dp, 1), "dp", 1)
    compressed = mm(
        lax.dynamic_slice_in_dim(own_normed, near, width_dp, 1), latent_shard, NT
    ) + swap(mm(far_normed, latent_shard, NT), "dp", 1)

    span_in = cube_gather(own_in, "experts")
    query_shard, far_normed = gate(query_proj, far_normed)
    query_other = swap(query_shard, "dp", 1)
    expand_shard, query_other = gate(expand_proj, query_other)
    expand_other = swap(expand_shard, "dp", 1)
    output_shard, expand_other = gate(output_proj, expand_other)
    output_other = swap(output_shard, "dp", 1)
    shared_shard, down_shard, latent_late, output_other = gate(
        shared_in.transpose(1, 2, 0).reshape(2 * shared_width, width_dp),
        shared_out,
        latent_shard,
        output_other,
    )
    shared_other = swap(shared_shard, "dp", 1)
    down_other = swap(down_shard, "dp", 1)
    latent_other = swap(latent_late, "dp", 1)
    query_proj = join_dp(query_shard, query_other, 0)
    expand_proj = join_dp(expand_shard, expand_other, 0)
    output_proj = join_dp(output_shard, output_other, 1)
    shared_in = join_dp(shared_shard, shared_other, 1)
    shared_out = join_dp(down_shard, down_other, 1)
    latent_proj = join_dp(latent_late, latent_other, 1)

    order = lax.dynamic_slice_in_dim(span_order, 2 * place_context, 2, 0)
    offsets = jnp.arange(rows_dev, dtype=jnp.int32)
    members = jnp.arange(count_experts, dtype=jnp.int32) ^ place_experts
    span_places = (members[:, None] * rows_dev + offsets[None, :]).reshape(span_rows)
    positions = (
        jnp.where(span_places < half, order[0], order[1]) * half + span_places % half
    )
    key_positions = (
        span_order[:, None] * half + jnp.arange(half, dtype=jnp.int32)[None, :]
    ).reshape(1, total_rows)
    cosine, sine = rope_tables(positions, ROPE)
    own_cosine, own_sine = cosine[:rows_dev], sine[:rows_dev]

    latent = compressed[:, :RANK]
    scale_latent = lax.rsqrt(jnp.mean(latent * latent, axis=1, keepdims=True) + eps_norm)
    latent_normed = (latent * scale_latent * latent_gain).astype(jnp.bfloat16)
    key_rope = rotate(compressed[:, RANK:], own_cosine, own_sine).astype(jnp.bfloat16)
    keys_all = lax.all_gather(
        jnp.concatenate([latent_normed, key_rope], axis=1),
        ("context", "experts"),
        axis=0,
        tiled=True,
    )
    latent_all, rope_all = keys_all[:, :RANK], keys_all[:, RANK:]

    span_float = span_in.astype(jnp.float32)
    scale_span = lax.rsqrt(jnp.mean(span_float * span_float, axis=1, keepdims=True) + eps_norm)
    normed = (span_float * scale_span * attn_gain).astype(jnp.bfloat16)
    query_raw = mm(normed, query_proj).reshape(span_rows, heads, NOPE + ROPE)
    q_nope = query_raw[:, :, :NOPE].reshape(span_rows, heads * NOPE).astype(jnp.bfloat16)
    q_rope = (
        rotate(query_raw[:, :, NOPE:], cosine[:, None, :], sine[:, None, :])
        .transpose(1, 0, 2)
        .astype(jnp.bfloat16)
    )
    keyvals = mm(latent_all, expand_proj).astype(jnp.bfloat16)
    q_pos = positions[:, None]
    attended, lse = attend_fwd(
        q_nope, q_rope, keyvals, rope_all, q_pos, key_positions, score_scale
    )
    hidden = inputs + cube_scatter(mm(attended, output_proj), "experts")
    scale_two = lax.rsqrt(jnp.mean(hidden * hidden, axis=1, keepdims=True) + eps_norm)
    hidden_normed = (hidden * scale_two * moe_gain).astype(jnp.bfloat16)

    gates = jax.nn.sigmoid(mm(hidden_normed, router_proj))
    picked = jnp.any(routes[0][:, :, None] == names[None, None, :], axis=1)
    chosen = jnp.where(picked, gates, 0.0)
    chosen_total = jnp.sum(chosen, axis=1, keepdims=True)
    route_weights = route_scale * chosen / chosen_total
    weights_high = route_weights.astype(jnp.bfloat16)
    weights_low = (route_weights - weights_high.astype(jnp.float32)).astype(jnp.bfloat16)
    code_width = -(-2 * experts // 128) * 128
    all_normed = lax.all_gather(
        jnp.concatenate(
            [
                hidden_normed,
                weights_high,
                weights_low,
                jnp.zeros((rows_dev, code_width - 2 * experts), jnp.bfloat16),
            ],
            axis=1,
        ),
        EVERY,
        axis=0,
        tiled=True,
    )

    capacity = rows_dev * TOPK * 4 // (3 * experts)
    name = place_context * count_experts + place_experts
    lower = (jnp.arange(rows_dev)[:, None] <= jnp.arange(rows_dev)[None, :]).astype(jnp.bfloat16)
    slots = jnp.arange(capacity, dtype=jnp.int32)
    hit = jnp.any(all_routes == name, axis=1).reshape(sources, rows_dev)
    ranks = mm(hit.astype(jnp.bfloat16), lower).astype(jnp.int32) - 1
    take_mask = hit[:, None, :] & (ranks[:, None, :] == slots[None, :, None])
    take = take_mask.astype(jnp.bfloat16)
    gate_up = expert_in[0].transpose(1, 2, 0).reshape(2 * width, D)
    down = expert_out[0]
    grads = pick_rows(take, [all_cot], D)
    bare_grad, all_normed = gate(mm(grads, down, NT), all_normed)

    all_codes = all_normed[:, D:].astype(jnp.float32)
    code_names = jnp.arange(code_width, dtype=jnp.int32)
    weight = jnp.sum(
        jnp.where(
            (code_names == name)[None, :] | (code_names == name + experts)[None, :], all_codes, 0.0
        ),
        axis=1,
    ).reshape(sources, rows_dev)
    slot_weight = jnp.sum(
        jnp.where(take_mask, weight[:, None, :], 0.0), axis=2
    ).reshape(sources * capacity, 1)
    rows = pick_rows(take, [all_normed], D)
    pre = mm(rows, gate_up, NT)
    act, pre_grad = gated_parts(pre[:, :width], pre[:, width:], bare_grad * slot_weight)
    weight_grad = jnp.sum(act.astype(jnp.float32) * bare_grad, axis=1, keepdims=True)
    act_weighted = (act.astype(jnp.float32) * slot_weight).astype(jnp.bfloat16)
    backs = mm(pre_grad, gate_up).astype(jnp.bfloat16)
    high = weight_grad.astype(jnp.bfloat16).astype(jnp.float32)
    back_width = -(-2 * count_dp * experts // 128) * 128
    columns = jnp.arange(back_width, dtype=jnp.int32)[None, :]
    column = place_dp * experts + name
    code = jnp.where(columns == column, high, 0.0) + jnp.where(
        columns == column + count_dp * experts, weight_grad - high, 0.0
    )
    tokens = sources * rows_dev
    piece = min(tokens, 4096)
    side = D // 2

    def scatter_every(values):
        return lax.psum_scatter(values, EVERY, scatter_dimension=0, tiled=True)

    code = code.astype(jnp.bfloat16)
    if tokens > piece:
        (back,) = place_rows(take, backs[:, :side], None, (side,))
        back, backs, code = gate(scatter_every(back), backs, code)
        (other,) = place_rows(take, backs[:, side:], code, (D - side,))
        back = jnp.concatenate([back, scatter_every(other)], axis=1)
    else:
        (back,) = place_rows(take, backs, code, (D,))
        back, all_normed, all_cot, pre_grad, rows, act_weighted, grads = gate(
            back, all_normed, all_cot, pre_grad, rows, act_weighted, grads
        )
        back = scatter_every(back)

    span_start = (place_dp * count_context + place_context) * span_rows

    def span_of(values):
        return jnp.concatenate(
            [
                lax.dynamic_slice_in_dim(
                    values, span_start + (place_experts ^ one) * rows_dev, rows_dev, 0
                )
                for one in range(count_experts)
            ],
            axis=0,
        )

    def shared_parts(normed_piece, cot_piece):
        shared_pre = mm(normed_piece, shared_in, NT)
        return gated_parts(
            shared_pre[:, :shared_width],
            shared_pre[:, shared_width:],
            mm(cot_piece, shared_out, NT),
        )

    if tokens > piece:
        all_normed, all_cot, back = gate(all_normed, all_cot, back)
        span_act, span_pre_grad = shared_parts(span_of(all_normed)[:, :D], span_of(all_cot))
        span_act, span_pre_grad, all_normed, all_cot = gate(
            span_act, span_pre_grad, all_normed, all_cot
        )
    shared_in_grad, shared_out_grad = 0.0, 0.0
    for start in range(0, tokens, piece):
        normed_piece = all_normed[start : start + piece, :D]
        cot_piece = all_cot[start : start + piece]
        shared_act, shared_pre_grad = shared_parts(normed_piece, cot_piece)
        shared_in_grad += mm(
            shared_pre_grad, lax.dynamic_slice_in_dim(normed_piece, near, width_dp, 1), TN
        )
        shared_out_grad += mm(
            shared_act, lax.dynamic_slice_in_dim(cot_piece, near, width_dp, 1), TN
        )
        if tokens > piece:
            shared_in_grad, shared_out_grad, all_normed, all_cot = gate(
                shared_in_grad, shared_out_grad, all_normed, all_cot
            )
        else:
            span_act, span_pre_grad = span_of(shared_act), span_of(shared_pre_grad)

    shared_sum = cube_scatter(
        jnp.concatenate(
            [
                mm(span_act, shared_out).astype(jnp.bfloat16),
                mm(span_pre_grad, shared_in).astype(jnp.bfloat16),
            ],
            axis=1,
        ),
        "experts",
    )
    expert_in_grad = mm(pre_grad, rows, TN)
    expert_out_grad = mm(act_weighted, grads, TN)
    back, shared_sum, shared_in_grad, shared_out_grad, expert_in_grad, expert_out_grad = gate(
        back, shared_sum, shared_in_grad, shared_out_grad, expert_in_grad, expert_out_grad
    )
    shared_in_grad = shared_in_grad.reshape(2, shared_width, width_dp).transpose(2, 0, 1)
    expert_in_grad = expert_in_grad.reshape(2, width, D).transpose(2, 0, 1)[None]
    expert_out_grad = expert_out_grad[None]
    back = back.astype(jnp.float32)

    codes = back[:, D : D + 2 * count_dp * experts].reshape(rows_dev, 2 * count_dp, experts)
    weight_grad = jnp.sum(codes, axis=1)
    chosen_grad = route_scale * weight_grad / chosen_total - route_scale * jnp.sum(
        weight_grad * chosen, axis=1, keepdims=True
    ) / (chosen_total * chosen_total)
    logit_grad = jnp.where(picked, chosen_grad * gates * (1.0 - gates), 0.0)
    normed_grad = (
        back[:, :D]
        + shared_sum[:, D:]
        + jnp.dot(
            logit_grad, router_proj.astype(jnp.float32).T, precision=lax.Precision.HIGHEST
        )
    )
    norm_part, moe_gain_grad = rms_back(normed_grad, hidden, scale_two, moe_gain)
    hidden_grad = own_cot.astype(jnp.float32) + norm_part
    outgoing, act_weighted = gate(hidden_grad.astype(jnp.bfloat16), act_weighted)
    hidden_round = cube_gather(outgoing, "experts")
    results = mm(act_weighted, down).astype(jnp.bfloat16)
    (forward_rows,) = place_rows(take, results, None, (D,))
    routed = scatter_every(forward_rows)

    def sum_heads(values):
        kept = lax.dynamic_slice_in_dim(values, near, width_dp, 0)
        sent = lax.dynamic_slice_in_dim(values, far, width_dp, 0)
        kept = (kept + swap(sent.astype(jnp.bfloat16), "dp", 1).astype(jnp.float32)).astype(
            jnp.bfloat16
        )
        return lax.psum_scatter(kept, "context", scatter_dimension=0, tiled=True)

    def full_heads(values):
        return lax.all_gather(values, "context", axis=0, tiled=True).astype(jnp.float32)

    attended_grad = mm(hidden_round, output_proj, NT).astype(jnp.bfloat16)
    output_part = sum_heads(mm(hidden_round, attended, TN))
    dq_nope, dq_rope, dkv, dkr = attend_bwd(
        q_nope,
        q_rope,
        keyvals,
        rope_all,
        q_pos,
        key_positions,
        attended,
        attended_grad,
        lse,
        score_scale,
    )
    latent_outgoing = jnp.concatenate([mm(dkv, expand_proj, NT).astype(jnp.bfloat16), dkr], axis=1)
    latent_part = lax.psum_scatter(
        latent_outgoing, ("context", "experts"), scatter_dimension=0, tiled=True
    ).astype(jnp.float32)
    dq_rope = rotate_back(dq_rope.transpose(1, 0, 2), cosine[:, None, :], sine[:, None, :])
    query_raw_grad = (
        jnp.concatenate([dq_nope.reshape(span_rows, heads, NOPE), dq_rope], axis=2)
        .reshape(span_rows, heads * (NOPE + ROPE))
        .astype(jnp.bfloat16)
    )
    head_grads = jnp.concatenate(
        [mm(normed, query_raw_grad, TN), mm(latent_all, dkv, TN).reshape(D, -1)], axis=1
    )
    head_grads = sum_heads(head_grads)
    input_part = cube_scatter(mm(query_raw_grad, query_proj, NT), "experts")

    latent_grad, latent_gain_grad = rms_back(
        latent_part[:, :RANK], latent, scale_latent, latent_gain
    )
    compressed_grad = jnp.concatenate(
        [latent_grad, rotate_back(latent_part[:, RANK:], own_cosine, own_sine)], axis=1
    ).astype(jnp.bfloat16)
    latent_proj_grad = mm(own_normed, compressed_grad, TN)
    kept = lax.dynamic_slice_in_dim(latent_proj_grad, near, width_dp, 0)
    sent = lax.dynamic_slice_in_dim(latent_proj_grad, far, width_dp, 0)
    kept = kept + swap(sent.astype(jnp.bfloat16), "dp", 1).astype(jnp.float32)
    latent_proj_grad = lax.psum_scatter(
        kept.astype(jnp.bfloat16), ("context", "experts"), scatter_dimension=0, tiled=True
    )
    latent_proj_grad = lax.all_gather(
        latent_proj_grad, ("context", "experts"), axis=0, tiled=True
    ).astype(jnp.float32)
    head_grads, output_proj_grad = full_heads(head_grads), full_heads(output_part).T
    query_wide = heads * (NOPE + ROPE)
    query_proj_grad = head_grads[:, :query_wide]
    expand_grad = head_grads[:, query_wide:].reshape(RANK // count_dp, -1)

    input_normed_grad = input_part + mm(compressed_grad, latent_proj)
    first_part, attn_gain_grad = rms_back(input_normed_grad, inputs, scale_one, attn_gain)
    input_grad = hidden_grad + first_part
    router_grad = jnp.dot(
        hidden_normed.astype(jnp.float32).T, logit_grad, precision=lax.Precision.HIGHEST
    )
    early = sum_everywhere(jnp.concatenate([moe_gain_grad, router_grad.reshape(-1)]))
    late = sum_everywhere(jnp.concatenate([attn_gain_grad, latent_gain_grad]))

    def part_dp(values, start, size):
        return lax.dynamic_slice_in_dim(values, start + place_dp * size, size, 0)

    block_output = hidden + routed.astype(jnp.float32) + shared_sum[:, :D]
    return (
        block_output[None],
        input_grad[None],
        part_dp(late, 0, cuts[0]),
        query_proj_grad,
        latent_proj_grad,
        part_dp(late, D, cuts[1]),
        expand_grad,
        output_proj_grad,
        part_dp(early, 0, cuts[2]),
        part_dp(early, D, cuts[3]).reshape(-1, experts),
        shared_in_grad,
        shared_out_grad,
        expert_in_grad,
        expert_out_grad,
    )


def solution(mesh):
    return jax.shard_map(
        layer,
        mesh=mesh,
        in_specs=(
            P("dp", ("context", "experts"), None),
            P("dp", ("context", "experts"), None),
            P("dp", ("context", "experts"), None),
            P(),
            P("dp"),
            P("dp", "experts"),
            P("dp", None),
            P("dp"),
            P("dp", "experts"),
            P("experts", "dp"),
            P("dp"),
            P("dp", None),
            P("dp", None, "experts"),
            P("experts", "dp"),
            P(("context", "experts"), None, None, "dp"),
            P(("context", "experts"), "dp", None),
        ),
        out_specs=(
            P("dp", ("context", "experts"), None),
            P("dp", ("context", "experts"), None),
            P("dp"),
            P("dp", "experts"),
            P("dp", None),
            P("dp"),
            P("dp", "experts"),
            P("experts", "dp"),
            P("dp"),
            P("dp", None),
            P("dp", None, "experts"),
            P("experts", "dp"),
            P(("context", "experts"), None, None, "dp"),
            P(("context", "experts"), "dp", None),
        ),
        check_vma=False,
    )
```

```python
import math

import jax
import jax.numpy as jnp
from jax import lax
from jax.experimental import pallas as pl
from jax.experimental.pallas import tpu as pltpu
from jax.sharding import PartitionSpec as P


D = 2048
NOPE = 128
ROPE = 64
VDIM = 128
RANK = 512
TOPK = 6


eps_norm = 1e-06
route_scale = 2.446
rope_base = 50000.0
masked_value = -1e30


def rope_tables(positions, width):
    count = width // 2
    exponents = jnp.arange(count, dtype=jnp.float32) * (2.0 / width)
    freqs = jnp.power(jnp.float32(rope_base), -exponents)
    angles = positions.astype(jnp.float32)[:, None] * freqs[None, :]
    cosine = jnp.cos(angles)
    sine = jnp.sin(angles)
    return (jnp.concatenate([cosine, cosine], axis=1), jnp.concatenate([sine, sine], axis=1))


def rotate(values, cosine, sine):
    count = values.shape[-1] // 2
    turned = jnp.concatenate([-values[..., count:], values[..., :count]], axis=-1)
    return values * cosine + turned * sine


def rotate_back(grads, cosine, sine):
    count = grads.shape[-1] // 2
    scaled = grads * sine
    turned = jnp.concatenate([scaled[..., count:], -scaled[..., :count]], axis=-1)
    return grads * cosine + turned


def rms_back(grad_normed, values, scale, gain):
    gained = grad_normed * gain
    gain_grad = jnp.sum(grad_normed * values * scale, axis=0)
    value_grad = scale * gained - values * (scale * scale * scale) * jnp.mean(
        gained * values, axis=1, keepdims=True
    )
    return (value_grad, gain_grad)


EVERY = ("dp", "context", "experts")
NT = (((1,), (1,)), ((), ()))
TN = (((0,), (0,)), ((), ()))


def mm(left, right, dims=None):
    if dims is None:
        return jnp.dot(left, right, preferred_element_type=jnp.float32)
    return lax.dot_general(left, right, dims, preferred_element_type=jnp.float32)


def gate(*values):
    return lax.optimization_barrier(values)


def swap(values, axis, mask):
    count = lax.axis_size(axis)
    return lax.ppermute(values, axis, [(i, i ^ mask) for i in range(count)])


def masks_of(axis):
    count = lax.axis_size(axis)
    return [1 << bit for bit in range(count.bit_length() - 1)]


def cube_gather(values, axis):
    held = {0: values}
    for mask in reversed(masks_of(axis)):
        keys = sorted(held)
        rows = values.shape[0]
        got = swap(jnp.concatenate([held[key] for key in keys], axis=0), axis, mask)
        for at, key in enumerate(keys):
            held[key | mask] = got[at * rows : (at + 1) * rows]
    return jnp.concatenate([held[key] for key in sorted(held)], axis=0)


def cube_scatter(values, axis):
    count = lax.axis_size(axis)
    rows = values.shape[0] // count
    held = {key: values[key * rows : (key + 1) * rows] for key in range(count)}
    for mask in masks_of(axis):
        kept = [key for key in sorted(held) if not key & mask]
        sent = jnp.concatenate([held[key | mask] for key in kept], axis=0)
        got = swap(sent.astype(jnp.bfloat16), axis, mask).astype(jnp.float32)
        held = {
            key: held[key].astype(jnp.float32) + got[at * rows : (at + 1) * rows]
            for at, key in enumerate(kept)
        }
    return held[0]


def bits_of(axes):
    return [(axis, mask) for axis in axes for mask in reversed(masks_of(axis))]


def bit_here(axis, mask):
    return (lax.axis_index(axis) // mask) % 2


def ordered_gather(values, axes):
    bits = bits_of(axes)
    shape = values.shape
    for at, (axis, mask) in enumerate(bits):
        got = swap(values, axis, mask)
        values = jnp.where(
            bit_here(axis, mask) == 0,
            jnp.stack([values, got], axis=at),
            jnp.stack([got, values], axis=at),
        )
    return values.reshape(-1, *shape[1:])


def scatter_stage(values, bits, stage, dtype):
    at = bits.index(stage)
    mine = bit_here(*stage)
    kept = lax.dynamic_index_in_dim(values, mine, at, keepdims=False)
    sent = lax.dynamic_index_in_dim(values, 1 - mine, at, keepdims=False)
    got = swap(sent.astype(jnp.bfloat16), *stage)
    total = kept.astype(jnp.float32) + got.astype(jnp.float32)
    return total.astype(dtype), bits[:at] + bits[at + 1 :]


def split_bits(values, bits):
    return values.reshape([2] * len(bits) + [-1, values.shape[-1]])


def ordered_scatter(values, axes, stages, dtype=jnp.float32):
    bits = bits_of(axes)
    values = split_bits(values, bits)
    for stage in stages:
        values, bits = scatter_stage(values, bits, stage, dtype)
    return values


def sum_everywhere(values):
    for axis in ("experts", "context", "dp"):
        for mask in masks_of(axis):
            values = values + swap(values, axis, mask)
    return values


def join_dp(values, other, axis):
    first = lax.axis_index("dp") == 0
    return jnp.where(
        first,
        jnp.concatenate([values, other], axis=axis),
        jnp.concatenate([other, values], axis=axis),
    )


def pick_rows(take, parts, width):
    sources, capacity, rows_dev = take.shape
    per = 4
    wide = [part.shape[1] for part in parts]

    def body(take_ref, *refs):
        out_ref = refs[-1]
        for one in range(per):
            start = 0
            for ref in refs[:-1]:
                span = min(ref.shape[1], width - start)
                out_ref[one * capacity : (one + 1) * capacity, start : start + span] = mm(
                    take_ref[one], ref[one * rows_dev : (one + 1) * rows_dev, :span]
                ).astype(jnp.bfloat16)
                start += span

    return pl.pallas_call(
        body,
        grid=(sources // per,),
        in_specs=[pl.BlockSpec((per, capacity, rows_dev), lambda s: (s, 0, 0))]
        + [pl.BlockSpec((per * rows_dev, size), lambda s: (s, 0)) for size in wide],
        out_specs=pl.BlockSpec((per * capacity, width), lambda s: (s, 0)),
        out_shape=jax.ShapeDtypeStruct((sources * capacity, width), jnp.bfloat16),
        compiler_params=pltpu.CompilerParams(vmem_limit_bytes=40 << 20),
        cost_estimate=pl.CostEstimate(
            flops=2 * sources * capacity * rows_dev * width,
            bytes_accessed=2 * sources * (rows_dev + capacity) * width,
            transcendentals=0,
        ),
        name="pick_rows",
    )(take, *parts)


def place_rows(take, values, extra, widths):
    sources, capacity, rows_dev = take.shape
    per = 4
    inputs = [values] if extra is None else [values, extra]
    shapes = list(widths)
    if extra is not None:
        shapes[-1] += extra.shape[1]

    def body(take_ref, *refs):
        ins, outs = refs[: len(inputs)], refs[len(inputs) :]
        for one in range(per):
            slots = slice(one * capacity, (one + 1) * capacity)
            rows = slice(one * rows_dev, (one + 1) * rows_dev)
            start = 0
            for ref, span in zip(outs, widths):
                ref[rows, :span] = mm(
                    take_ref[one], ins[0][slots, start : start + span], TN
                ).astype(jnp.bfloat16)
                start += span
            if extra is not None:
                outs[-1][rows, widths[-1] :] = mm(take_ref[one], ins[1][slots, :], TN).astype(
                    jnp.bfloat16
                )

    return pl.pallas_call(
        body,
        grid=(sources // per,),
        in_specs=[pl.BlockSpec((per, capacity, rows_dev), lambda s: (s, 0, 0))]
        + [pl.BlockSpec((per * capacity, one.shape[1]), lambda s: (s, 0)) for one in inputs],
        out_specs=[pl.BlockSpec((per * rows_dev, size), lambda s: (s, 0)) for size in shapes],
        out_shape=[
            jax.ShapeDtypeStruct((sources * rows_dev, size), jnp.bfloat16) for size in shapes
        ],
        compiler_params=pltpu.CompilerParams(vmem_limit_bytes=40 << 20),
        cost_estimate=pl.CostEstimate(
            flops=2 * sources * capacity * rows_dev * sum(shapes),
            bytes_accessed=2 * sources * (rows_dev + capacity) * sum(shapes),
            transcendentals=0,
        ),
        name="place_rows",
    )(take, *inputs)


def gated_parts(gate, upper, act_grad):
    sig = jax.nn.sigmoid(gate)
    act = (gate * sig * upper).astype(jnp.bfloat16)
    pre_grad = jnp.concatenate(
        [act_grad * upper * sig * (1.0 + gate * (1.0 - sig)), act_grad * gate * sig], axis=1
    ).astype(jnp.bfloat16)
    return act, pre_grad


def attend_fwd_body(scale, qn_ref, qr_ref, kv_ref, kr_ref, qp_ref, kp_ref, out_ref, lse_ref):
    scores = mm(qn_ref[...], kv_ref[:, :NOPE], NT) + mm(qr_ref[0], kr_ref[...], NT)
    scores = jnp.where(kp_ref[...] <= qp_ref[...], scores * scale, masked_value)
    top = jnp.max(scores, axis=1, keepdims=True)
    weights = jnp.exp(scores - top)
    total = jnp.sum(weights, axis=1, keepdims=True)
    out = mm(weights.astype(jnp.bfloat16), kv_ref[:, NOPE:])
    out_ref[...] = (out / total).astype(jnp.bfloat16)
    lse_ref[0] = top + jnp.log(total)


def attend_fwd(q_nope, q_rope, keyvals, rope_keys, q_pos, k_pos, scale):
    heads, rows, rope = q_rope.shape
    keys = keyvals.shape[0]
    tile = min(rows, 256)
    return pl.pallas_call(
        lambda *refs: attend_fwd_body(scale, *refs),
        grid=(heads, rows // tile),
        in_specs=[
            pl.BlockSpec((tile, NOPE), lambda h, i: (i, h)),
            pl.BlockSpec((1, tile, rope), lambda h, i: (h, i, 0)),
            pl.BlockSpec((keys, NOPE + VDIM), lambda h, i: (0, h)),
            pl.BlockSpec((keys, rope), lambda h, i: (0, 0)),
            pl.BlockSpec((tile, 1), lambda h, i: (i, 0)),
            pl.BlockSpec((1, keys), lambda h, i: (0, 0)),
        ],
        out_specs=[
            pl.BlockSpec((tile, VDIM), lambda h, i: (i, h)),
            pl.BlockSpec((1, tile, 1), lambda h, i: (h, i, 0)),
        ],
        out_shape=[
            jax.ShapeDtypeStruct((rows, heads * VDIM), jnp.bfloat16),
            jax.ShapeDtypeStruct((heads, rows, 1), jnp.float32),
        ],
        compiler_params=pltpu.CompilerParams(vmem_limit_bytes=60 << 20),
        cost_estimate=pl.CostEstimate(
            flops=2 * heads * rows * keys * (NOPE + rope + VDIM),
            bytes_accessed=4 * keys * heads * (NOPE + VDIM),
            transcendentals=heads * rows * keys,
        ),
        name="attend_fwd",
    )(q_nope, q_rope, keyvals, rope_keys, q_pos, k_pos)


def attend_bwd_body(
    scale,
    qn_ref,
    qr_ref,
    kv_ref,
    kr_ref,
    qp_ref,
    kp_ref,
    out_ref,
    grad_ref,
    lse_ref,
    dqn_ref,
    dqr_ref,
    dkv_ref,
    dkr_ref,
    dk_sum,
    dv_sum,
    dr_sum,
):
    head, tile = pl.program_id(1), pl.program_id(2)
    tiles = pl.num_programs(2)
    grad = grad_ref[...]
    q_nope, q_rope = qn_ref[...], qr_ref[0]
    keys, values = kv_ref[:, :NOPE], kv_ref[:, NOPE:]
    scores = mm(q_nope, keys, NT) + mm(q_rope, kr_ref[...], NT)
    probs = jnp.exp(scores * scale - lse_ref[0])
    probs = jnp.where(kp_ref[...] <= qp_ref[...], probs, 0.0)
    delta = jnp.sum(
        out_ref[...].astype(jnp.float32) * grad.astype(jnp.float32), axis=1, keepdims=True
    )
    score_grad = (probs * (mm(grad, values, NT) - delta)).astype(jnp.bfloat16)
    dqn_ref[0] = scale * mm(score_grad, keys)
    dqr_ref[0, 0] = scale * mm(score_grad, kr_ref[...])
    key_part = mm(score_grad, q_nope, TN)
    value_part = mm(probs.astype(jnp.bfloat16), grad, TN)
    rope_part = mm(score_grad, q_rope, TN)

    @pl.when(tile == 0)
    def _():
        dk_sum[...] = key_part
        dv_sum[...] = value_part

    @pl.when(tile > 0)
    def _():
        dk_sum[...] += key_part
        dv_sum[...] += value_part

    @pl.when((tile == 0) & (head == 0))
    def _():
        dr_sum[...] = rope_part

    @pl.when((tile > 0) | (head > 0))
    def _():
        dr_sum[...] += rope_part

    @pl.when(tile == tiles - 1)
    def _():
        dkv_ref[:, :NOPE] = (scale * dk_sum[...]).astype(jnp.bfloat16)
        dkv_ref[:, NOPE:] = dv_sum[...].astype(jnp.bfloat16)

    @pl.when((tile == tiles - 1) & (head == pl.num_programs(1) - 1))
    def _():
        dkr_ref[...] = (scale * dr_sum[...]).astype(jnp.bfloat16)


def attend_bwd(q_nope, q_rope, keyvals, rope_keys, q_pos, k_pos, attended, grad, lse, scale):
    heads, rows, rope = q_rope.shape
    keys = keyvals.shape[0]
    tile = min(rows, 256)
    chunk = min(keys, 2048)
    chunks = keys // chunk
    dqn, dqr, dkv, dkr = pl.pallas_call(
        lambda *refs: attend_bwd_body(scale, *refs),
        grid=(chunks, heads, rows // tile),
        in_specs=[
            pl.BlockSpec((tile, NOPE), lambda c, h, i: (i, h)),
            pl.BlockSpec((1, tile, rope), lambda c, h, i: (h, i, 0)),
            pl.BlockSpec((chunk, NOPE + VDIM), lambda c, h, i: (c, h)),
            pl.BlockSpec((chunk, rope), lambda c, h, i: (c, 0)),
            pl.BlockSpec((tile, 1), lambda c, h, i: (i, 0)),
            pl.BlockSpec((1, chunk), lambda c, h, i: (0, c)),
            pl.BlockSpec((tile, VDIM), lambda c, h, i: (i, h)),
            pl.BlockSpec((tile, VDIM), lambda c, h, i: (i, h)),
            pl.BlockSpec((1, tile, 1), lambda c, h, i: (h, i, 0)),
        ],
        out_specs=[
            pl.BlockSpec((1, tile, NOPE), lambda c, h, i: (c, i, h)),
            pl.BlockSpec((1, 1, tile, rope), lambda c, h, i: (c, h, i, 0)),
            pl.BlockSpec((chunk, NOPE + VDIM), lambda c, h, i: (c, h)),
            pl.BlockSpec((chunk, rope), lambda c, h, i: (c, 0)),
        ],
        out_shape=[
            jax.ShapeDtypeStruct((chunks, rows, heads * NOPE), jnp.float32),
            jax.ShapeDtypeStruct((chunks, heads, rows, rope), jnp.float32),
            jax.ShapeDtypeStruct((keys, heads * (NOPE + VDIM)), jnp.bfloat16),
            jax.ShapeDtypeStruct((keys, rope), jnp.bfloat16),
        ],
        scratch_shapes=[
            pltpu.VMEM((chunk, NOPE), jnp.float32),
            pltpu.VMEM((chunk, VDIM), jnp.float32),
            pltpu.VMEM((chunk, rope), jnp.float32),
        ],
        compiler_params=pltpu.CompilerParams(vmem_limit_bytes=60 << 20),
        cost_estimate=pl.CostEstimate(
            flops=2 * heads * rows * keys * (3 * NOPE + 3 * rope + 2 * VDIM),
            bytes_accessed=8 * keys * heads * (NOPE + VDIM),
            transcendentals=heads * rows * keys,
        ),
        name="attend_bwd",
    )(q_nope, q_rope, keyvals, rope_keys, q_pos, k_pos, attended, grad, lse)
    return jnp.sum(dqn, axis=0), jnp.sum(dqr, axis=0), dkv, dkr


def layer(
    layer_input,
    cotangent,
    routes,
    span_order,
    attn_gain,
    query_proj,
    latent_proj,
    latent_gain,
    expand_proj,
    output_proj,
    moe_gain,
    router_proj,
    shared_in,
    shared_out,
    expert_in,
    expert_out,
):
    place_dp = lax.axis_index("dp")
    place_context = lax.axis_index("context")
    place_experts = lax.axis_index("experts")
    count_dp = lax.axis_size("dp")
    count_context = lax.axis_size("context")
    count_experts = lax.axis_size("experts")
    own_in = layer_input[0]
    own_cot = cotangent[0]
    rows_dev = own_in.shape[0]
    sources = count_dp * count_context * count_experts
    heads = query_proj.shape[1] // (NOPE + ROPE)
    experts = router_proj.shape[1]
    shared_width = shared_out.shape[0]
    width = expert_out.shape[1]
    score_scale = 1.0 / math.sqrt(NOPE + ROPE)

    span_rows = count_experts * rows_dev
    total_rows = span_rows * count_context
    half = span_rows // 2
    width_dp = D // count_dp
    near = place_dp * width_dp
    far = (1 - place_dp) * width_dp

    names = jnp.arange(experts, dtype=jnp.int32)
    route_code = jnp.pad(routes[0], ((0, 0), (0, 128 - TOPK))).astype(jnp.bfloat16)
    all_routes = ordered_gather(route_code, EVERY)
    all_routes = all_routes[:, :TOPK].astype(jnp.int32)
    tokens = sources * rows_dev
    piece = min(tokens, 4096)
    if tokens > piece:
        all_cot = lax.all_gather(own_cot, EVERY, axis=0, tiled=True)
    else:
        all_cot = ordered_gather(own_cot, EVERY)

    small = jnp.concatenate([attn_gain, latent_gain, moe_gain, router_proj.reshape(-1)])
    cuts = [attn_gain.size, latent_gain.size, moe_gain.size, router_proj.size]
    starts = [sum(cuts[:i]) for i in range(4)]
    small = join_dp(small[None], swap(small, "dp", 1)[None], 0)
    attn_gain, latent_gain, moe_gain, router_flat = (
        small[:, start : start + size].reshape(-1) for start, size in zip(starts, cuts)
    )
    router_proj = router_flat.reshape(-1, experts)
    attn_gain, latent_gain, moe_gain = (
        gain.astype(jnp.float32) for gain in (attn_gain, latent_gain, moe_gain)
    )

    inputs = own_in.astype(jnp.float32)
    scale_one = lax.rsqrt(jnp.mean(inputs * inputs, axis=1, keepdims=True) + eps_norm)
    own_normed = (inputs * scale_one * attn_gain).astype(jnp.bfloat16)
    latent_shard = latent_proj.T
    far_normed = swap(lax.dynamic_slice_in_dim(own_normed, far, width_dp, 1), "dp", 1)
    far_part = mm(far_normed, latent_shard, NT)
    compressed = mm(
        lax.dynamic_slice_in_dim(own_normed, near, width_dp, 1), latent_shard, NT
    ) + swap(far_part, "dp", 1)

    span_in = cube_gather(own_in, "experts")
    query_shard, far_normed = gate(query_proj, far_normed)
    query_other = swap(query_shard, "dp", 1)
    expand_shard, query_other = gate(expand_proj, query_other)
    expand_other = swap(expand_shard, "dp", 1)
    output_shard, expand_other = gate(output_proj, expand_other)
    output_other = swap(output_shard, "dp", 1)
    shared_shard, down_shard, latent_late, output_other = gate(
        shared_in.transpose(1, 2, 0).reshape(2 * shared_width, width_dp),
        shared_out,
        latent_shard,
        output_other,
    )
    shared_other = swap(shared_shard, "dp", 1)
    down_other = swap(down_shard, "dp", 1)
    latent_other = swap(latent_late, "dp", 1)
    query_proj = join_dp(query_shard, query_other, 0)
    expand_proj = join_dp(expand_shard, expand_other, 0)
    output_proj = join_dp(output_shard, output_other, 1)
    shared_in = join_dp(shared_shard, shared_other, 1)
    shared_out = join_dp(down_shard, down_other, 1)
    latent_proj = join_dp(latent_late, latent_other, 1)

    order = lax.dynamic_slice_in_dim(span_order, 2 * place_context, 2, 0)
    offsets = jnp.arange(rows_dev, dtype=jnp.int32)
    members = jnp.arange(count_experts, dtype=jnp.int32) ^ place_experts
    span_places = (members[:, None] * rows_dev + offsets[None, :]).reshape(span_rows)
    positions = (
        jnp.where(span_places < half, order[0], order[1]) * half + span_places % half
    )
    key_positions = (
        span_order[:, None] * half + jnp.arange(half, dtype=jnp.int32)[None, :]
    ).reshape(1, total_rows)
    cosine, sine = rope_tables(positions, ROPE)
    own_cosine, own_sine = cosine[:rows_dev], sine[:rows_dev]

    latent = compressed[:, :RANK]
    scale_latent = lax.rsqrt(jnp.mean(latent * latent, axis=1, keepdims=True) + eps_norm)
    latent_normed = (latent * scale_latent * latent_gain).astype(jnp.bfloat16)
    key_rope = rotate(compressed[:, RANK:], own_cosine, own_sine).astype(jnp.bfloat16)
    keys_all = lax.all_gather(
        jnp.concatenate([latent_normed, key_rope], axis=1),
        ("context", "experts"),
        axis=0,
        tiled=True,
    )
    latent_all, rope_all = keys_all[:, :RANK], keys_all[:, RANK:]

    span_float = span_in.astype(jnp.float32)
    scale_span = lax.rsqrt(jnp.mean(span_float * span_float, axis=1, keepdims=True) + eps_norm)
    normed = (span_float * scale_span * attn_gain).astype(jnp.bfloat16)
    query_raw = mm(normed, query_proj)
    query_raw = query_raw.reshape(span_rows, heads, NOPE + ROPE)
    q_nope = query_raw[:, :, :NOPE].reshape(span_rows, heads * NOPE).astype(jnp.bfloat16)
    q_rope = (
        rotate(query_raw[:, :, NOPE:], cosine[:, None, :], sine[:, None, :])
        .transpose(1, 0, 2)
        .astype(jnp.bfloat16)
    )
    keyvals = mm(latent_all, expand_proj).astype(jnp.bfloat16)
    q_pos = positions[:, None]
    attended, lse = attend_fwd(
        q_nope, q_rope, keyvals, rope_all, q_pos, key_positions, score_scale
    )
    mixed = mm(attended, output_proj)
    hidden = inputs + cube_scatter(mixed, "experts")
    scale_two = lax.rsqrt(jnp.mean(hidden * hidden, axis=1, keepdims=True) + eps_norm)
    hidden_normed = (hidden * scale_two * moe_gain).astype(jnp.bfloat16)

    gates = mm(hidden_normed, router_proj)
    gates = jax.nn.sigmoid(gates)
    picked = jnp.any(routes[0][:, :, None] == names[None, None, :], axis=1)
    chosen = jnp.where(picked, gates, 0.0)
    chosen_total = jnp.sum(chosen, axis=1, keepdims=True)
    route_weights = route_scale * chosen / chosen_total
    weights_high = route_weights.astype(jnp.bfloat16)
    weights_low = (route_weights - weights_high.astype(jnp.float32)).astype(jnp.bfloat16)
    code_width = -(-2 * experts // 128) * 128
    all_normed = lax.all_gather(
        jnp.concatenate(
            [
                hidden_normed,
                weights_high,
                weights_low,
                jnp.zeros((rows_dev, code_width - 2 * experts), jnp.bfloat16),
            ],
            axis=1,
        ),
        EVERY,
        axis=0,
        tiled=True,
    )

    capacity = rows_dev * TOPK * 4 // (3 * experts)
    name = place_context * count_experts + place_experts
    lower = (jnp.arange(rows_dev)[:, None] <= jnp.arange(rows_dev)[None, :]).astype(jnp.bfloat16)
    slots = jnp.arange(capacity, dtype=jnp.int32)
    hit = jnp.any(all_routes == name, axis=1).reshape(sources, rows_dev)
    ranks = mm(hit.astype(jnp.bfloat16), lower).astype(jnp.int32) - 1
    take_mask = hit[:, None, :] & (ranks[:, None, :] == slots[None, :, None])
    take = take_mask.astype(jnp.bfloat16)
    gate_up = expert_in[0].transpose(1, 2, 0).reshape(2 * width, D)
    down = expert_out[0]
    grads = pick_rows(take, [all_cot], D)
    bare_grad, all_normed = gate(mm(grads, down, NT), all_normed)

    all_codes = all_normed[:, D:].astype(jnp.float32)
    code_names = jnp.arange(code_width, dtype=jnp.int32)
    weight = jnp.sum(
        jnp.where(
            (code_names == name)[None, :] | (code_names == name + experts)[None, :], all_codes, 0.0
        ),
        axis=1,
    ).reshape(sources, rows_dev)
    slot_weight = jnp.sum(
        jnp.where(take_mask, weight[:, None, :], 0.0), axis=2
    ).reshape(sources * capacity, 1)
    rows = pick_rows(take, [all_normed], D)
    pre = mm(rows, gate_up, NT)
    act, pre_grad = gated_parts(pre[:, :width], pre[:, width:], bare_grad * slot_weight)
    weight_grad = jnp.sum(act.astype(jnp.float32) * bare_grad, axis=1, keepdims=True)
    act_weighted = (act.astype(jnp.float32) * slot_weight).astype(jnp.bfloat16)
    backs = mm(pre_grad, gate_up).astype(jnp.bfloat16)
    high = weight_grad.astype(jnp.bfloat16).astype(jnp.float32)
    back_width = -(-2 * count_dp * experts // 128) * 128
    columns = jnp.arange(back_width, dtype=jnp.int32)[None, :]
    column = place_dp * experts + name
    code = jnp.where(columns == column, high, 0.0) + jnp.where(
        columns == column + count_dp * experts, weight_grad - high, 0.0
    )
    side = D // 2

    def scatter_every(values):
        return lax.psum_scatter(values, EVERY, scatter_dimension=0, tiled=True)

    code = code.astype(jnp.bfloat16)
    if tokens > piece:
        (back,) = place_rows(take, backs[:, :side], None, (side,))
        back, backs, code = gate(scatter_every(back), backs, code)
        (other,) = place_rows(take, backs[:, side:], code, (D - side,))
        back = jnp.concatenate([back, scatter_every(other)], axis=1)
    else:
        (back,) = place_rows(take, backs, code, (D,))
        back, all_normed, all_cot, pre_grad, rows, act_weighted, grads = gate(
            back, all_normed, all_cot, pre_grad, rows, act_weighted, grads
        )
        back = scatter_every(back)

    span_start = (place_dp * count_context + place_context) * span_rows

    def span_of(values):
        return jnp.concatenate(
            [
                lax.dynamic_slice_in_dim(
                    values, span_start + (place_experts ^ one) * rows_dev, rows_dev, 0
                )
                for one in range(count_experts)
            ],
            axis=0,
        )

    def shared_parts(normed_piece, cot_piece):
        shared_pre = mm(normed_piece, shared_in, NT)
        return gated_parts(
            shared_pre[:, :shared_width],
            shared_pre[:, shared_width:],
            mm(cot_piece, shared_out, NT),
        )

    if tokens > piece:
        all_normed, all_cot, back = gate(all_normed, all_cot, back)
        span_act, span_pre_grad = shared_parts(span_of(all_normed)[:, :D], span_of(all_cot))
        span_act, span_pre_grad, all_normed, all_cot = gate(
            span_act, span_pre_grad, all_normed, all_cot
        )
    shared_in_grad, shared_out_grad = 0.0, 0.0
    for start in range(0, tokens, piece):
        normed_piece = all_normed[start : start + piece, :D]
        cot_piece = all_cot[start : start + piece]
        shared_act, shared_pre_grad = shared_parts(normed_piece, cot_piece)
        shared_in_grad += mm(
            shared_pre_grad, lax.dynamic_slice_in_dim(normed_piece, near, width_dp, 1), TN
        )
        shared_out_grad += mm(
            shared_act, lax.dynamic_slice_in_dim(cot_piece, near, width_dp, 1), TN
        )
        if tokens > piece:
            shared_in_grad, shared_out_grad, all_normed, all_cot = gate(
                shared_in_grad, shared_out_grad, all_normed, all_cot
            )
        else:
            span_act, span_pre_grad = span_of(shared_act), span_of(shared_pre_grad)

    shared_sum = cube_scatter(
        jnp.concatenate(
            [
                mm(span_act, shared_out).astype(jnp.bfloat16),
                mm(span_pre_grad, shared_in).astype(jnp.bfloat16),
            ],
            axis=1,
        ),
        "experts",
    )
    expert_in_grad = mm(pre_grad, rows, TN)
    expert_out_grad = mm(act_weighted, grads, TN)
    back, shared_sum, shared_in_grad, shared_out_grad, expert_in_grad, expert_out_grad = gate(
        back, shared_sum, shared_in_grad, shared_out_grad, expert_in_grad, expert_out_grad
    )
    shared_in_grad = shared_in_grad.reshape(2, shared_width, width_dp).transpose(2, 0, 1)
    expert_in_grad = expert_in_grad.reshape(2, width, D).transpose(2, 0, 1)[None]
    expert_out_grad = expert_out_grad[None]
    back = back.astype(jnp.float32)

    codes = back[:, D : D + 2 * count_dp * experts].reshape(rows_dev, 2 * count_dp, experts)
    weight_grad = jnp.sum(codes, axis=1)
    chosen_grad = route_scale * weight_grad / chosen_total - route_scale * jnp.sum(
        weight_grad * chosen, axis=1, keepdims=True
    ) / (chosen_total * chosen_total)
    logit_grad = jnp.where(picked, chosen_grad * gates * (1.0 - gates), 0.0)
    normed_grad = (
        back[:, :D]
        + shared_sum[:, D:]
        + jnp.dot(
            logit_grad, router_proj.astype(jnp.float32).T, precision=lax.Precision.HIGHEST
        )
    )
    norm_part, moe_gain_grad = rms_back(normed_grad, hidden, scale_two, moe_gain)
    hidden_grad = own_cot.astype(jnp.float32) + norm_part
    outgoing, act_weighted = gate(hidden_grad.astype(jnp.bfloat16), act_weighted)
    hidden_round = cube_gather(outgoing, "experts")
    results = mm(act_weighted, down).astype(jnp.bfloat16)
    every_bits = bits_of(EVERY)
    inner = [bit for bit in every_bits if bit[0] == "experts"][::-1]
    along = [bit for bit in every_bits if bit[0] == "context"][::-1]
    across = [bit for bit in every_bits if bit[0] == "dp"]
    orders = (
        inner[:1] + inner[1:] + across + along,
        inner[:1] + along + across + inner[1:],
    )
    if tokens > piece:
        (forward_rows,) = place_rows(take, results, None, (D,))
        routed = scatter_every(forward_rows)
    else:
        halves = []
        for part, values in enumerate(place_rows(take, results, None, (side, D - side))):
            halves.append(
                scatter_stage(
                    split_bits(values, every_bits), every_bits, orders[part][0], jnp.bfloat16
                )
            )
        hidden_round, first_half, second_half = gate(hidden_round, halves[0][0], halves[1][0])
        routed = []
        for part, values in enumerate((first_half, second_half)):
            bits = halves[part][1]
            for stage in orders[part][1:]:
                values, bits = scatter_stage(values, bits, stage, jnp.bfloat16)
            routed.append(values)
        routed = jnp.concatenate(routed, axis=1)

    def sum_heads(values):
        kept = lax.dynamic_slice_in_dim(values, near, width_dp, 0)
        sent = lax.dynamic_slice_in_dim(values, far, width_dp, 0)
        kept = (kept + swap(sent.astype(jnp.bfloat16), "dp", 1).astype(jnp.float32)).astype(
            jnp.bfloat16
        )
        return lax.psum_scatter(kept, "context", scatter_dimension=0, tiled=True)

    def full_heads(values):
        return lax.all_gather(values, "context", axis=0, tiled=True).astype(jnp.float32)

    attended_grad = mm(hidden_round, output_proj, NT).astype(jnp.bfloat16)
    output_part = sum_heads(mm(hidden_round, attended, TN))
    dq_nope, dq_rope, dkv, dkr = attend_bwd(
        q_nope,
        q_rope,
        keyvals,
        rope_all,
        q_pos,
        key_positions,
        attended,
        attended_grad,
        lse,
        score_scale,
    )
    latent_outgoing = jnp.concatenate([mm(dkv, expand_proj, NT).astype(jnp.bfloat16), dkr], axis=1)
    latent_part = ordered_scatter(latent_outgoing, ("context", "experts"), inner + along)
    dq_rope = rotate_back(dq_rope.transpose(1, 0, 2), cosine[:, None, :], sine[:, None, :])
    query_raw_grad = (
        jnp.concatenate([dq_nope.reshape(span_rows, heads, NOPE), dq_rope], axis=2)
        .reshape(span_rows, heads * (NOPE + ROPE))
        .astype(jnp.bfloat16)
    )
    query_wide_grad = mm(normed, query_raw_grad, TN)
    head_grads = jnp.concatenate(
        [query_wide_grad, mm(latent_all, dkv, TN).reshape(D, -1)], axis=1
    )
    head_grads = sum_heads(head_grads)
    input_part = cube_scatter(mm(query_raw_grad, query_proj, NT), "experts")

    latent_grad, latent_gain_grad = rms_back(
        latent_part[:, :RANK], latent, scale_latent, latent_gain
    )
    compressed_grad = jnp.concatenate(
        [latent_grad, rotate_back(latent_part[:, RANK:], own_cosine, own_sine)], axis=1
    ).astype(jnp.bfloat16)
    latent_proj_grad = mm(own_normed, compressed_grad, TN)
    latent_proj_grad = ordered_scatter(latent_proj_grad, EVERY, inner + along + across)
    latent_proj_grad = ordered_gather(
        latent_proj_grad.astype(jnp.bfloat16), ("context", "experts")
    ).astype(jnp.float32)
    head_grads, output_proj_grad = full_heads(head_grads), full_heads(output_part).T
    query_wide = heads * (NOPE + ROPE)
    query_proj_grad = head_grads[:, :query_wide]
    expand_grad = head_grads[:, query_wide:].reshape(RANK // count_dp, -1)

    input_normed_grad = input_part + mm(compressed_grad, latent_proj)
    first_part, attn_gain_grad = rms_back(input_normed_grad, inputs, scale_one, attn_gain)
    input_grad = hidden_grad + first_part
    router_grad = jnp.dot(
        hidden_normed.astype(jnp.float32).T, logit_grad, precision=lax.Precision.HIGHEST
    )
    early = sum_everywhere(jnp.concatenate([moe_gain_grad, router_grad.reshape(-1)]))
    late = sum_everywhere(jnp.concatenate([attn_gain_grad, latent_gain_grad]))

    def part_dp(values, start, size):
        return lax.dynamic_slice_in_dim(values, start + place_dp * size, size, 0)

    block_output = hidden + routed.astype(jnp.float32) + shared_sum[:, :D]
    return (
        block_output[None],
        input_grad[None],
        part_dp(late, 0, cuts[0]),
        query_proj_grad,
        latent_proj_grad,
        part_dp(late, D, cuts[1]),
        expand_grad,
        output_proj_grad,
        part_dp(early, 0, cuts[2]),
        part_dp(early, D, cuts[3]).reshape(-1, experts),
        shared_in_grad,
        shared_out_grad,
        expert_in_grad,
        expert_out_grad,
    )


def solution(mesh):
    return jax.shard_map(
        layer,
        mesh=mesh,
        in_specs=(
            P("dp", ("context", "experts"), None),
            P("dp", ("context", "experts"), None),
            P("dp", ("context", "experts"), None),
            P(),
            P("dp"),
            P("dp", "experts"),
            P("dp", None),
            P("dp"),
            P("dp", "experts"),
            P("experts", "dp"),
            P("dp"),
            P("dp", None),
            P("dp", None, "experts"),
            P("experts", "dp"),
            P(("context", "experts"), None, None, "dp"),
            P(("context", "experts"), "dp", None),
        ),
        out_specs=(
            P("dp", ("context", "experts"), None),
            P("dp", ("context", "experts"), None),
            P("dp"),
            P("dp", "experts"),
            P("dp", None),
            P("dp"),
            P("dp", "experts"),
            P("experts", "dp"),
            P("dp"),
            P("dp", None),
            P("dp", None, "experts"),
            P("experts", "dp"),
            P(("context", "experts"), None, None, "dp"),
            P(("context", "experts"), "dp", None),
        ),
        check_vma=False,
    )
```

```python
import math

import jax
import jax.numpy as jnp
from jax import lax
from jax.experimental import pallas as pl
from jax.experimental.pallas import tpu as pltpu
from jax.sharding import PartitionSpec as P


D = 2048
NOPE = 128
ROPE = 64
VDIM = 128
RANK = 512
TOPK = 6


eps_norm = 1e-06
route_scale = 2.446
rope_base = 50000.0
masked_value = -1e30


def rope_tables(positions, width):
    count = width // 2
    exponents = jnp.arange(count, dtype=jnp.float32) * (2.0 / width)
    freqs = jnp.power(jnp.float32(rope_base), -exponents)
    angles = positions.astype(jnp.float32)[:, None] * freqs[None, :]
    cosine = jnp.cos(angles)
    sine = jnp.sin(angles)
    return (jnp.concatenate([cosine, cosine], axis=1), jnp.concatenate([sine, sine], axis=1))


def rotate(values, cosine, sine):
    count = values.shape[-1] // 2
    turned = jnp.concatenate([-values[..., count:], values[..., :count]], axis=-1)
    return values * cosine + turned * sine


def rotate_back(grads, cosine, sine):
    count = grads.shape[-1] // 2
    scaled = grads * sine
    turned = jnp.concatenate([scaled[..., count:], -scaled[..., :count]], axis=-1)
    return grads * cosine + turned


def rms_back(grad_normed, values, scale, gain):
    gained = grad_normed * gain
    gain_grad = jnp.sum(grad_normed * values * scale, axis=0)
    value_grad = scale * gained - values * (scale * scale * scale) * jnp.mean(
        gained * values, axis=1, keepdims=True
    )
    return (value_grad, gain_grad)


EVERY = ("dp", "context", "experts")
INNER = EVERY[1:]
NT = (((1,), (1,)), ((), ()))
TN = (((0,), (0,)), ((), ()))


def mm(left, right, dims=None):
    if dims is None:
        return jnp.dot(left, right, preferred_element_type=jnp.float32)
    return lax.dot_general(left, right, dims, preferred_element_type=jnp.float32)


def gate(*values):
    return lax.optimization_barrier(values)


def swap(values, axis, mask):
    count = lax.axis_size(axis)
    return lax.ppermute(values, axis, [(i, i ^ mask) for i in range(count)])


def masks_of(axis):
    count = lax.axis_size(axis)
    return [1 << bit for bit in range(count.bit_length() - 1)]


def cube_gather(values, axis):
    held = {0: values}
    for mask in reversed(masks_of(axis)):
        keys = sorted(held)
        rows = values.shape[0]
        got = swap(jnp.concatenate([held[key] for key in keys], axis=0), axis, mask)
        for at, key in enumerate(keys):
            held[key | mask] = got[at * rows : (at + 1) * rows]
    return jnp.concatenate([held[key] for key in sorted(held)], axis=0)


def cube_scatter(values, axis):
    count = lax.axis_size(axis)
    rows = values.shape[0] // count
    held = {key: values[key * rows : (key + 1) * rows] for key in range(count)}
    for mask in masks_of(axis):
        kept = [key for key in sorted(held) if not key & mask]
        sent = jnp.concatenate([held[key | mask] for key in kept], axis=0)
        got = swap(sent.astype(jnp.bfloat16), axis, mask).astype(jnp.float32)
        held = {
            key: held[key].astype(jnp.float32) + got[at * rows : (at + 1) * rows]
            for at, key in enumerate(kept)
        }
    return held[0]


def bits_of(axes):
    return [(axis, mask) for axis in axes for mask in reversed(masks_of(axis))]


def bit_here(axis, mask):
    return (lax.axis_index(axis) // mask) % 2


def ordered_gather(values, axes):
    bits = bits_of(axes)
    shape = values.shape
    for at, (axis, mask) in enumerate(bits):
        got = swap(values, axis, mask)
        values = jnp.where(
            bit_here(axis, mask) == 0,
            jnp.stack([values, got], axis=at),
            jnp.stack([got, values], axis=at),
        )
    return values.reshape(-1, *shape[1:])


def scatter_stage(values, bits, stage, dtype):
    at = bits.index(stage)
    mine = bit_here(*stage)
    kept = lax.dynamic_index_in_dim(values, mine, at, keepdims=False)
    sent = lax.dynamic_index_in_dim(values, 1 - mine, at, keepdims=False)
    got = swap(sent.astype(jnp.bfloat16), *stage)
    total = kept.astype(jnp.float32) + got.astype(jnp.float32)
    return total.astype(dtype), bits[:at] + bits[at + 1 :]


def split_bits(values, bits):
    return values.reshape([2] * len(bits) + [-1, values.shape[-1]])


def ordered_scatter(values, axes, stages, dtype=jnp.float32):
    bits = bits_of(axes)
    values = split_bits(values, bits)
    for stage in stages:
        values, bits = scatter_stage(values, bits, stage, dtype)
    return values


def sum_everywhere(values):
    for axis in ("experts", "context", "dp"):
        for mask in masks_of(axis):
            values = values + swap(values, axis, mask)
    return values


def join_dp(values, other, axis):
    first = lax.axis_index("dp") == 0
    return jnp.where(
        first,
        jnp.concatenate([values, other], axis=axis),
        jnp.concatenate([other, values], axis=axis),
    )


def pick_rows(take, parts, width):
    sources, capacity, rows_dev = take.shape
    per = 4
    wide = [part.shape[1] for part in parts]

    def body(take_ref, *refs):
        out_ref = refs[-1]
        for one in range(per):
            start = 0
            for ref in refs[:-1]:
                span = min(ref.shape[1], width - start)
                out_ref[one * capacity : (one + 1) * capacity, start : start + span] = mm(
                    take_ref[one], ref[one * rows_dev : (one + 1) * rows_dev, :span]
                ).astype(jnp.bfloat16)
                start += span

    return pl.pallas_call(
        body,
        grid=(sources // per,),
        in_specs=[pl.BlockSpec((per, capacity, rows_dev), lambda s: (s, 0, 0))]
        + [pl.BlockSpec((per * rows_dev, size), lambda s: (s, 0)) for size in wide],
        out_specs=pl.BlockSpec((per * capacity, width), lambda s: (s, 0)),
        out_shape=jax.ShapeDtypeStruct((sources * capacity, width), jnp.bfloat16),
        compiler_params=pltpu.CompilerParams(vmem_limit_bytes=40 << 20),
        cost_estimate=pl.CostEstimate(
            flops=2 * sources * capacity * rows_dev * width,
            bytes_accessed=2 * sources * (rows_dev + capacity) * width,
            transcendentals=0,
        ),
        name="pick",
    )(take, *parts)


def place_rows(take, values, extra, widths):
    sources, capacity, rows_dev = take.shape
    per = 4
    inputs = [values] if extra is None else [values, extra]
    shapes = list(widths)
    if extra is not None:
        shapes[-1] += extra.shape[1]

    def body(take_ref, *refs):
        ins, outs = refs[: len(inputs)], refs[len(inputs) :]
        for one in range(per):
            slots = slice(one * capacity, (one + 1) * capacity)
            rows = slice(one * rows_dev, (one + 1) * rows_dev)
            start = 0
            for ref, span in zip(outs, widths):
                ref[rows, :span] = mm(
                    take_ref[one], ins[0][slots, start : start + span], TN
                ).astype(jnp.bfloat16)
                start += span
            if extra is not None:
                outs[-1][rows, widths[-1] :] = mm(take_ref[one], ins[1][slots, :], TN).astype(
                    jnp.bfloat16
                )

    return pl.pallas_call(
        body,
        grid=(sources // per,),
        in_specs=[pl.BlockSpec((per, capacity, rows_dev), lambda s: (s, 0, 0))]
        + [pl.BlockSpec((per * capacity, one.shape[1]), lambda s: (s, 0)) for one in inputs],
        out_specs=[pl.BlockSpec((per * rows_dev, size), lambda s: (s, 0)) for size in shapes],
        out_shape=[
            jax.ShapeDtypeStruct((sources * rows_dev, size), jnp.bfloat16) for size in shapes
        ],
        compiler_params=pltpu.CompilerParams(vmem_limit_bytes=40 << 20),
        cost_estimate=pl.CostEstimate(
            flops=2 * sources * capacity * rows_dev * sum(shapes),
            bytes_accessed=2 * sources * (rows_dev + capacity) * sum(shapes),
            transcendentals=0,
        ),
        name="place",
    )(take, *inputs)


def gated_parts(gate, upper, act_grad):
    sig = jax.nn.sigmoid(gate)
    act = (gate * sig * upper).astype(jnp.bfloat16)
    pre_grad = jnp.concatenate(
        [act_grad * upper * sig * (1.0 + gate * (1.0 - sig)), act_grad * gate * sig], axis=1
    ).astype(jnp.bfloat16)
    return act, pre_grad


def attend_fwd_body(scale, qn_ref, qr_ref, kv_ref, kr_ref, qp_ref, kp_ref, out_ref, lse_ref):
    scores = mm(qn_ref[...], kv_ref[:, :NOPE], NT) + mm(qr_ref[0], kr_ref[...], NT)
    scores = jnp.where(kp_ref[...] <= qp_ref[...], scores * scale, masked_value)
    top = jnp.max(scores, axis=1, keepdims=True)
    weights = jnp.exp(scores - top)
    total = jnp.sum(weights, axis=1, keepdims=True)
    out = mm(weights.astype(jnp.bfloat16), kv_ref[:, NOPE:])
    out_ref[...] = (out / total).astype(jnp.bfloat16)
    lse_ref[0] = top + jnp.log(total)


def attend_fwd(q_nope, q_rope, keyvals, rope_keys, q_pos, k_pos, scale):
    heads, rows, rope = q_rope.shape
    keys = keyvals.shape[0]
    tile = min(rows, 256)
    return pl.pallas_call(
        lambda *refs: attend_fwd_body(scale, *refs),
        grid=(heads, rows // tile),
        in_specs=[
            pl.BlockSpec((tile, NOPE), lambda h, i: (i, h)),
            pl.BlockSpec((1, tile, rope), lambda h, i: (h, i, 0)),
            pl.BlockSpec((keys, NOPE + VDIM), lambda h, i: (0, h)),
            pl.BlockSpec((keys, rope), lambda h, i: (0, 0)),
            pl.BlockSpec((tile, 1), lambda h, i: (i, 0)),
            pl.BlockSpec((1, keys), lambda h, i: (0, 0)),
        ],
        out_specs=[
            pl.BlockSpec((tile, VDIM), lambda h, i: (i, h)),
            pl.BlockSpec((1, tile, 1), lambda h, i: (h, i, 0)),
        ],
        out_shape=[
            jax.ShapeDtypeStruct((rows, heads * VDIM), jnp.bfloat16),
            jax.ShapeDtypeStruct((heads, rows, 1), jnp.float32),
        ],
        compiler_params=pltpu.CompilerParams(vmem_limit_bytes=60 << 20),
        cost_estimate=pl.CostEstimate(
            flops=2 * heads * rows * keys * (NOPE + rope + VDIM),
            bytes_accessed=4 * keys * heads * (NOPE + VDIM),
            transcendentals=heads * rows * keys,
        ),
        name="af",
    )(q_nope, q_rope, keyvals, rope_keys, q_pos, k_pos)


def attend_bwd_body(
    scale,
    qn_ref,
    qr_ref,
    kv_ref,
    kr_ref,
    qp_ref,
    kp_ref,
    out_ref,
    grad_ref,
    lse_ref,
    dqn_ref,
    dqr_ref,
    dkv_ref,
    dkr_ref,
    dk_sum,
    dv_sum,
    dr_sum,
):
    head, tile = pl.program_id(1), pl.program_id(2)
    tiles = pl.num_programs(2)
    grad = grad_ref[...]
    q_nope, q_rope = qn_ref[...], qr_ref[0]
    keys, values = kv_ref[:, :NOPE], kv_ref[:, NOPE:]
    scores = mm(q_nope, keys, NT) + mm(q_rope, kr_ref[...], NT)
    probs = jnp.exp(scores * scale - lse_ref[0])
    probs = jnp.where(kp_ref[...] <= qp_ref[...], probs, 0.0)
    delta = jnp.sum(
        out_ref[...].astype(jnp.float32) * grad.astype(jnp.float32), axis=1, keepdims=True
    )
    score_grad = (probs * (mm(grad, values, NT) - delta)).astype(jnp.bfloat16)
    dqn_ref[0] = scale * mm(score_grad, keys)
    dqr_ref[0, 0] = scale * mm(score_grad, kr_ref[...])
    key_part = mm(score_grad, q_nope, TN)
    value_part = mm(probs.astype(jnp.bfloat16), grad, TN)
    rope_part = mm(score_grad, q_rope, TN)

    @pl.when(tile == 0)
    def _():
        dk_sum[...] = key_part
        dv_sum[...] = value_part

    @pl.when(tile > 0)
    def _():
        dk_sum[...] += key_part
        dv_sum[...] += value_part

    @pl.when((tile == 0) & (head == 0))
    def _():
        dr_sum[...] = rope_part

    @pl.when((tile > 0) | (head > 0))
    def _():
        dr_sum[...] += rope_part

    @pl.when(tile == tiles - 1)
    def _():
        dkv_ref[:, :NOPE] = (scale * dk_sum[...]).astype(jnp.bfloat16)
        dkv_ref[:, NOPE:] = dv_sum[...].astype(jnp.bfloat16)

    @pl.when((tile == tiles - 1) & (head == pl.num_programs(1) - 1))
    def _():
        dkr_ref[...] = (scale * dr_sum[...]).astype(jnp.bfloat16)


def attend_bwd(q_nope, q_rope, keyvals, rope_keys, q_pos, k_pos, attended, grad, lse, scale):
    heads, rows, rope = q_rope.shape
    keys = keyvals.shape[0]
    tile = min(rows, 256)
    chunk = min(keys, 2048)
    chunks = keys // chunk
    dqn, dqr, dkv, dkr = pl.pallas_call(
        lambda *refs: attend_bwd_body(scale, *refs),
        grid=(chunks, heads, rows // tile),
        in_specs=[
            pl.BlockSpec((tile, NOPE), lambda c, h, i: (i, h)),
            pl.BlockSpec((1, tile, rope), lambda c, h, i: (h, i, 0)),
            pl.BlockSpec((chunk, NOPE + VDIM), lambda c, h, i: (c, h)),
            pl.BlockSpec((chunk, rope), lambda c, h, i: (c, 0)),
            pl.BlockSpec((tile, 1), lambda c, h, i: (i, 0)),
            pl.BlockSpec((1, chunk), lambda c, h, i: (0, c)),
            pl.BlockSpec((tile, VDIM), lambda c, h, i: (i, h)),
            pl.BlockSpec((tile, VDIM), lambda c, h, i: (i, h)),
            pl.BlockSpec((1, tile, 1), lambda c, h, i: (h, i, 0)),
        ],
        out_specs=[
            pl.BlockSpec((1, tile, NOPE), lambda c, h, i: (c, i, h)),
            pl.BlockSpec((1, 1, tile, rope), lambda c, h, i: (c, h, i, 0)),
            pl.BlockSpec((chunk, NOPE + VDIM), lambda c, h, i: (c, h)),
            pl.BlockSpec((chunk, rope), lambda c, h, i: (c, 0)),
        ],
        out_shape=[
            jax.ShapeDtypeStruct((chunks, rows, heads * NOPE), jnp.float32),
            jax.ShapeDtypeStruct((chunks, heads, rows, rope), jnp.float32),
            jax.ShapeDtypeStruct((keys, heads * (NOPE + VDIM)), jnp.bfloat16),
            jax.ShapeDtypeStruct((keys, rope), jnp.bfloat16),
        ],
        scratch_shapes=[
            pltpu.VMEM((chunk, NOPE), jnp.float32),
            pltpu.VMEM((chunk, VDIM), jnp.float32),
            pltpu.VMEM((chunk, rope), jnp.float32),
        ],
        compiler_params=pltpu.CompilerParams(vmem_limit_bytes=60 << 20),
        cost_estimate=pl.CostEstimate(
            flops=2 * heads * rows * keys * (3 * NOPE + 3 * rope + 2 * VDIM),
            bytes_accessed=8 * keys * heads * (NOPE + VDIM),
            transcendentals=heads * rows * keys,
        ),
        name="ab",
    )(q_nope, q_rope, keyvals, rope_keys, q_pos, k_pos, attended, grad, lse)
    return jnp.sum(dqn, axis=0), jnp.sum(dqr, axis=0), dkv, dkr


def layer(
    layer_input,
    cotangent,
    routes,
    span_order,
    attn_gain,
    query_proj,
    latent_proj,
    latent_gain,
    expand_proj,
    output_proj,
    moe_gain,
    router_proj,
    shared_in,
    shared_out,
    expert_in,
    expert_out,
):
    place_dp = lax.axis_index("dp")
    place_context = lax.axis_index("context")
    place_experts = lax.axis_index("experts")
    count_dp = lax.axis_size("dp")
    count_context = lax.axis_size("context")
    count_experts = lax.axis_size("experts")
    own_in = layer_input[0]
    own_cot = cotangent[0]
    rows_dev = own_in.shape[0]
    sources = count_dp * count_context * count_experts
    heads = query_proj.shape[1] // (NOPE + ROPE)
    experts = router_proj.shape[1]
    shared_width = shared_out.shape[0]
    width = expert_out.shape[1]
    score_scale = 1.0 / math.sqrt(NOPE + ROPE)

    span_rows = count_experts * rows_dev
    total_rows = span_rows * count_context
    half = span_rows // 2
    width_dp = D // count_dp
    near = place_dp * width_dp
    far = (1 - place_dp) * width_dp

    names = jnp.arange(experts, dtype=jnp.int32)
    route_code = jnp.pad(routes[0], ((0, 0), (0, 128 - TOPK))).astype(jnp.bfloat16)
    all_routes = ordered_gather(route_code, EVERY)
    all_routes = all_routes[:, :TOPK].astype(jnp.int32)
    tokens = sources * rows_dev
    piece = min(tokens, 4096)
    all_cot = lax.all_gather(own_cot, EVERY, axis=0, tiled=True)

    small = jnp.concatenate([attn_gain, latent_gain, moe_gain, router_proj.reshape(-1)])
    cuts = [attn_gain.size, latent_gain.size, moe_gain.size, router_proj.size]
    starts = [sum(cuts[:i]) for i in range(4)]
    small = join_dp(small[None], swap(small, "dp", 1)[None], 0)
    attn_gain, latent_gain, moe_gain, router_flat = (
        small[:, start : start + size].reshape(-1) for start, size in zip(starts, cuts)
    )
    router_proj = router_flat.reshape(-1, experts)
    attn_gain, latent_gain, moe_gain = (
        gain.astype(jnp.float32) for gain in (attn_gain, latent_gain, moe_gain)
    )

    inputs = own_in.astype(jnp.float32)
    scale_one = lax.rsqrt(jnp.mean(inputs * inputs, axis=1, keepdims=True) + eps_norm)
    own_normed = (inputs * scale_one * attn_gain).astype(jnp.bfloat16)
    latent_shard = latent_proj.T
    far_normed = swap(lax.dynamic_slice_in_dim(own_normed, far, width_dp, 1), "dp", 1)
    far_part = mm(far_normed, latent_shard, NT)
    compressed = mm(
        lax.dynamic_slice_in_dim(own_normed, near, width_dp, 1), latent_shard, NT
    ) + swap(far_part, "dp", 1)

    span_in = cube_gather(own_in, "experts")
    query_shard, far_normed = gate(query_proj, far_normed)
    query_other = swap(query_shard, "dp", 1)
    expand_shard, query_other = gate(expand_proj, query_other)
    expand_other = swap(expand_shard, "dp", 1)
    output_shard, expand_other = gate(output_proj, expand_other)
    output_other = swap(output_shard, "dp", 1)
    shared_shard, down_shard, latent_late, output_other = gate(
        shared_in.transpose(1, 2, 0).reshape(2 * shared_width, width_dp),
        shared_out,
        latent_shard,
        output_other,
    )
    shared_other = swap(shared_shard, "dp", 1)
    down_other = swap(down_shard, "dp", 1)
    latent_other = swap(latent_late, "dp", 1)
    query_proj = join_dp(query_shard, query_other, 0)
    expand_proj = join_dp(expand_shard, expand_other, 0)
    output_proj = join_dp(output_shard, output_other, 1)
    shared_in = join_dp(shared_shard, shared_other, 1)
    shared_out = join_dp(down_shard, down_other, 1)
    latent_proj = join_dp(latent_late, latent_other, 1)

    order = lax.dynamic_slice_in_dim(span_order, 2 * place_context, 2, 0)
    offsets = jnp.arange(rows_dev, dtype=jnp.int32)
    members = jnp.arange(count_experts, dtype=jnp.int32) ^ place_experts
    span_places = (members[:, None] * rows_dev + offsets[None, :]).reshape(span_rows)
    positions = (
        jnp.where(span_places < half, order[0], order[1]) * half + span_places % half
    )
    key_positions = (
        span_order[:, None] * half + jnp.arange(half, dtype=jnp.int32)[None, :]
    ).reshape(1, total_rows)
    cosine, sine = rope_tables(positions, ROPE)
    own_cosine, own_sine = cosine[:rows_dev], sine[:rows_dev]

    latent = compressed[:, :RANK]
    scale_latent = lax.rsqrt(jnp.mean(latent * latent, axis=1, keepdims=True) + eps_norm)
    latent_normed = (latent * scale_latent * latent_gain).astype(jnp.bfloat16)
    key_rope = rotate(compressed[:, RANK:], own_cosine, own_sine).astype(jnp.bfloat16)
    keys_all = ordered_gather(jnp.concatenate([latent_normed, key_rope], axis=1), INNER)
    latent_all, rope_all = keys_all[:, :RANK], keys_all[:, RANK:]

    span_float = span_in.astype(jnp.float32)
    scale_span = lax.rsqrt(jnp.mean(span_float * span_float, axis=1, keepdims=True) + eps_norm)
    normed = (span_float * scale_span * attn_gain).astype(jnp.bfloat16)
    query_raw = mm(normed, query_proj)
    query_raw = query_raw.reshape(span_rows, heads, NOPE + ROPE)
    q_nope = query_raw[:, :, :NOPE].reshape(span_rows, heads * NOPE).astype(jnp.bfloat16)
    q_rope = (
        rotate(query_raw[:, :, NOPE:], cosine[:, None, :], sine[:, None, :])
        .transpose(1, 0, 2)
        .astype(jnp.bfloat16)
    )
    keyvals = mm(latent_all, expand_proj).astype(jnp.bfloat16)
    q_pos = positions[:, None]
    attended, lse = attend_fwd(
        q_nope, q_rope, keyvals, rope_all, q_pos, key_positions, score_scale
    )
    mixed = mm(attended, output_proj)
    hidden = inputs + cube_scatter(mixed, "experts")
    scale_two = lax.rsqrt(jnp.mean(hidden * hidden, axis=1, keepdims=True) + eps_norm)
    hidden_normed = (hidden * scale_two * moe_gain).astype(jnp.bfloat16)

    gates = jax.nn.sigmoid(mm(hidden_normed, router_proj))
    picked = jnp.any(routes[0][:, :, None] == names[None, None, :], axis=1)
    chosen = jnp.where(picked, gates, 0.0)
    chosen_total = jnp.sum(chosen, axis=1, keepdims=True)
    route_weights = route_scale * chosen / chosen_total
    weights_high = route_weights.astype(jnp.bfloat16)
    weights_low = (route_weights - weights_high.astype(jnp.float32)).astype(jnp.bfloat16)
    code_width = -(-2 * experts // 128) * 128
    all_normed = lax.all_gather(
        jnp.concatenate(
            [
                hidden_normed,
                weights_high,
                weights_low,
                jnp.zeros((rows_dev, code_width - 2 * experts), jnp.bfloat16),
            ],
            axis=1,
        ),
        EVERY,
        axis=0,
        tiled=True,
    )

    capacity = rows_dev * TOPK * 4 // (3 * experts)
    name = place_context * count_experts + place_experts
    lower = (jnp.arange(rows_dev)[:, None] <= jnp.arange(rows_dev)[None, :]).astype(jnp.bfloat16)
    slots = jnp.arange(capacity, dtype=jnp.int32)
    hit = jnp.any(all_routes == name, axis=1).reshape(sources, rows_dev)
    ranks = mm(hit.astype(jnp.bfloat16), lower).astype(jnp.int32) - 1
    take_mask = hit[:, None, :] & (ranks[:, None, :] == slots[None, :, None])
    take = take_mask.astype(jnp.bfloat16)
    gate_up = expert_in[0].transpose(1, 2, 0).reshape(2 * width, D)
    down = expert_out[0]
    grads = pick_rows(take, [all_cot], D)
    bare_grad, all_normed = gate(mm(grads, down, NT), all_normed)

    all_codes = all_normed[:, D:].astype(jnp.float32)
    code_names = jnp.arange(code_width, dtype=jnp.int32)
    weight = jnp.sum(
        jnp.where(
            (code_names == name)[None, :] | (code_names == name + experts)[None, :], all_codes, 0.0
        ),
        axis=1,
    ).reshape(sources, rows_dev)
    slot_weight = jnp.sum(
        jnp.where(take_mask, weight[:, None, :], 0.0), axis=2
    ).reshape(sources * capacity, 1)
    rows = pick_rows(take, [all_normed], D)
    pre = mm(rows, gate_up, NT)
    act, pre_grad = gated_parts(pre[:, :width], pre[:, width:], bare_grad * slot_weight)
    weight_grad = jnp.sum(act.astype(jnp.float32) * bare_grad, axis=1, keepdims=True)
    act_weighted = (act.astype(jnp.float32) * slot_weight).astype(jnp.bfloat16)
    backs = mm(pre_grad, gate_up).astype(jnp.bfloat16)
    high = weight_grad.astype(jnp.bfloat16).astype(jnp.float32)
    back_width = -(-2 * count_dp * experts // 128) * 128
    columns = jnp.arange(back_width, dtype=jnp.int32)[None, :]
    column = place_dp * experts + name
    code = jnp.where(columns == column, high, 0.0) + jnp.where(
        columns == column + count_dp * experts, weight_grad - high, 0.0
    )
    side = D // 2

    def scatter_every(values):
        return lax.psum_scatter(values, EVERY, scatter_dimension=0, tiled=True)

    code = code.astype(jnp.bfloat16)
    if tokens > piece:
        (back,) = place_rows(take, backs[:, :side], None, (side,))
        back, backs, code = gate(scatter_every(back), backs, code)
        (other,) = place_rows(take, backs[:, side:], code, (D - side,))
        back = jnp.concatenate([back, scatter_every(other)], axis=1)
    else:
        (back,) = place_rows(take, backs, code, (D,))
        back, all_normed, all_cot, pre_grad, rows, act_weighted, grads = gate(
            back, all_normed, all_cot, pre_grad, rows, act_weighted, grads
        )
        back = scatter_every(back)

    span_start = (place_dp * count_context + place_context) * span_rows

    def span_of(values):
        return jnp.concatenate(
            [
                lax.dynamic_slice_in_dim(
                    values, span_start + (place_experts ^ one) * rows_dev, rows_dev, 0
                )
                for one in range(count_experts)
            ],
            axis=0,
        )

    def shared_parts(normed_piece, cot_piece):
        shared_pre = mm(normed_piece, shared_in, NT)
        return gated_parts(
            shared_pre[:, :shared_width],
            shared_pre[:, shared_width:],
            mm(cot_piece, shared_out, NT),
        )

    if tokens > piece:
        all_normed, all_cot, back = gate(all_normed, all_cot, back)
        span_act, span_pre_grad = shared_parts(span_of(all_normed)[:, :D], span_of(all_cot))
        span_act, span_pre_grad, all_normed, all_cot = gate(
            span_act, span_pre_grad, all_normed, all_cot
        )
    shared_in_grad, shared_out_grad = 0.0, 0.0
    for start in range(0, tokens, piece):
        normed_piece = all_normed[start : start + piece, :D]
        cot_piece = all_cot[start : start + piece]
        shared_act, shared_pre_grad = shared_parts(normed_piece, cot_piece)
        shared_in_grad += mm(
            shared_pre_grad, lax.dynamic_slice_in_dim(normed_piece, near, width_dp, 1), TN
        )
        shared_out_grad += mm(
            shared_act, lax.dynamic_slice_in_dim(cot_piece, near, width_dp, 1), TN
        )
        if tokens > piece:
            shared_in_grad, shared_out_grad, all_normed, all_cot = gate(
                shared_in_grad, shared_out_grad, all_normed, all_cot
            )
        else:
            span_act, span_pre_grad = span_of(shared_act), span_of(shared_pre_grad)

    shared_sum = cube_scatter(
        jnp.concatenate(
            [
                mm(span_act, shared_out).astype(jnp.bfloat16),
                mm(span_pre_grad, shared_in).astype(jnp.bfloat16),
            ],
            axis=1,
        ),
        "experts",
    )
    expert_in_grad = mm(pre_grad, rows, TN)
    expert_out_grad = mm(act_weighted, grads, TN)
    back, shared_sum, shared_in_grad, shared_out_grad, expert_in_grad, expert_out_grad = gate(
        back, shared_sum, shared_in_grad, shared_out_grad, expert_in_grad, expert_out_grad
    )
    shared_in_grad = shared_in_grad.reshape(2, shared_width, width_dp).transpose(2, 0, 1)
    expert_in_grad = expert_in_grad.reshape(2, width, D).transpose(2, 0, 1)[None]
    expert_out_grad = expert_out_grad[None]
    back = back.astype(jnp.float32)

    codes = back[:, D : D + 2 * count_dp * experts].reshape(rows_dev, 2 * count_dp, experts)
    weight_grad = jnp.sum(codes, axis=1)
    chosen_grad = route_scale * weight_grad / chosen_total - route_scale * jnp.sum(
        weight_grad * chosen, axis=1, keepdims=True
    ) / (chosen_total * chosen_total)
    logit_grad = jnp.where(picked, chosen_grad * gates * (1.0 - gates), 0.0)
    normed_grad = (
        back[:, :D]
        + shared_sum[:, D:]
        + jnp.dot(
            logit_grad, router_proj.astype(jnp.float32).T, precision=lax.Precision.HIGHEST
        )
    )
    norm_part, moe_gain_grad = rms_back(normed_grad, hidden, scale_two, moe_gain)
    hidden_grad = own_cot.astype(jnp.float32) + norm_part
    outgoing, act_weighted = gate(hidden_grad.astype(jnp.bfloat16), act_weighted)
    hidden_round = cube_gather(outgoing, "experts")
    results = mm(act_weighted, down).astype(jnp.bfloat16)
    every_bits = bits_of(EVERY)
    inner = [bit for bit in every_bits if bit[0] == "experts"][::-1]
    along = [bit for bit in every_bits if bit[0] == "context"][::-1]
    across = [bit for bit in every_bits if bit[0] == "dp"]
    orders = (
        inner[:1] + inner[1:] + across + along,
        inner[:1] + along + across + inner[1:],
    )
    if tokens > piece:
        (forward_rows,) = place_rows(take, results, None, (D,))
        routed = scatter_every(forward_rows)
    else:
        halves = []
        for part, values in enumerate(place_rows(take, results, None, (side, D - side))):
            halves.append(
                scatter_stage(
                    split_bits(values, every_bits), every_bits, orders[part][0], jnp.bfloat16
                )
            )
        hidden_round, first_half, second_half = gate(hidden_round, halves[0][0], halves[1][0])
        routed = []
        for part, values in enumerate((first_half, second_half)):
            bits = halves[part][1]
            for stage in orders[part][1:]:
                values, bits = scatter_stage(values, bits, stage, jnp.bfloat16)
            routed.append(values)
        routed = jnp.concatenate(routed, axis=1)

    def sum_heads(values):
        kept = lax.dynamic_slice_in_dim(values, near, width_dp, 0)
        sent = lax.dynamic_slice_in_dim(values, far, width_dp, 0)
        got = swap(sent.astype(jnp.bfloat16), "dp", 1)
        kept = (kept + got.astype(jnp.float32)).astype(jnp.bfloat16)
        return lax.psum_scatter(kept, "context", scatter_dimension=0, tiled=True)

    def full_heads(values):
        return lax.all_gather(values, "context", axis=0, tiled=True).astype(jnp.float32)

    attended_grad = mm(hidden_round, output_proj, NT).astype(jnp.bfloat16)
    output_part = sum_heads(mm(hidden_round, attended, TN))
    dq_nope, dq_rope, dkv, dkr = attend_bwd(
        q_nope,
        q_rope,
        keyvals,
        rope_all,
        q_pos,
        key_positions,
        attended,
        attended_grad,
        lse,
        score_scale,
    )
    dq_rope = rotate_back(dq_rope.transpose(1, 0, 2), cosine[:, None, :], sine[:, None, :])
    query_raw_grad = (
        jnp.concatenate([dq_nope.reshape(span_rows, heads, NOPE), dq_rope], axis=2)
        .reshape(span_rows, heads * (NOPE + ROPE))
        .astype(jnp.bfloat16)
    )
    head_grads = jnp.concatenate(
        [mm(normed, query_raw_grad, TN), mm(latent_all, dkv, TN).reshape(D, -1)], axis=1
    )
    head_grads, dkv, query_raw_grad = gate(head_grads, dkv, query_raw_grad)
    head_grads = sum_heads(head_grads)
    latent_outgoing = mm(dkv, expand_proj, NT).astype(jnp.bfloat16)
    latent_outgoing = jnp.concatenate([latent_outgoing, dkr], axis=1)
    latent_part = ordered_scatter(latent_outgoing, INNER, inner + along)
    input_part = cube_scatter(mm(query_raw_grad, query_proj, NT), "experts")

    latent_grad, latent_gain_grad = rms_back(
        latent_part[:, :RANK], latent, scale_latent, latent_gain
    )
    compressed_grad = jnp.concatenate(
        [latent_grad, rotate_back(latent_part[:, RANK:], own_cosine, own_sine)], axis=1
    ).astype(jnp.bfloat16)
    latent_proj_grad = mm(own_normed, compressed_grad, TN).astype(jnp.bfloat16)
    latent_proj_grad = lax.all_gather(
        scatter_every(latent_proj_grad), INNER, axis=0, tiled=True
    ).astype(jnp.float32)
    head_grads, output_proj_grad = full_heads(head_grads), full_heads(output_part).T
    query_wide = heads * (NOPE + ROPE)
    query_proj_grad = head_grads[:, :query_wide]
    expand_grad = head_grads[:, query_wide:].reshape(RANK // count_dp, -1)

    input_normed_grad = input_part + mm(compressed_grad, latent_proj)
    first_part, attn_gain_grad = rms_back(input_normed_grad, inputs, scale_one, attn_gain)
    input_grad = hidden_grad + first_part
    router_grad = jnp.dot(
        hidden_normed.astype(jnp.float32).T, logit_grad, precision=lax.Precision.HIGHEST
    )
    early = sum_everywhere(jnp.concatenate([moe_gain_grad, router_grad.reshape(-1)]))
    late = sum_everywhere(jnp.concatenate([attn_gain_grad, latent_gain_grad]))

    def part_dp(values, start, size):
        return lax.dynamic_slice_in_dim(values, start + place_dp * size, size, 0)

    block_output = hidden + routed.astype(jnp.float32) + shared_sum[:, :D]
    return (
        block_output[None],
        input_grad[None],
        part_dp(late, 0, cuts[0]),
        query_proj_grad,
        latent_proj_grad,
        part_dp(late, D, cuts[1]),
        expand_grad,
        output_proj_grad,
        part_dp(early, 0, cuts[2]),
        part_dp(early, D, cuts[3]).reshape(-1, experts),
        shared_in_grad,
        shared_out_grad,
        expert_in_grad,
        expert_out_grad,
    )


def solution(mesh):
    return jax.shard_map(
        layer,
        mesh=mesh,
        in_specs=(
            P("dp", ("context", "experts"), None),
            P("dp", ("context", "experts"), None),
            P("dp", ("context", "experts"), None),
            P(),
            P("dp"),
            P("dp", "experts"),
            P("dp", None),
            P("dp"),
            P("dp", "experts"),
            P("experts", "dp"),
            P("dp"),
            P("dp", None),
            P("dp", None, "experts"),
            P("experts", "dp"),
            P(("context", "experts"), None, None, "dp"),
            P(("context", "experts"), "dp", None),
        ),
        out_specs=(
            P("dp", ("context", "experts"), None),
            P("dp", ("context", "experts"), None),
            P("dp"),
            P("dp", "experts"),
            P("dp", None),
            P("dp"),
            P("dp", "experts"),
            P("experts", "dp"),
            P("dp"),
            P("dp", None),
            P("dp", None, "experts"),
            P("experts", "dp"),
            P(("context", "experts"), None, None, "dp"),
            P(("context", "experts"), "dp", None),
        ),
        check_vma=False,
    )
```

```python
import math

import jax
import jax.numpy as jnp
from jax import lax
from jax.experimental import pallas as pl
from jax.experimental.pallas import tpu as pltpu
from jax.sharding import PartitionSpec as P


D = 2048
NOPE = 128
ROPE = 64
VDIM = 128
RANK = 512
TOPK = 6


eps_norm = 1e-06
route_scale = 2.446
rope_base = 50000.0
masked_value = -1e30


def rope_tables(positions, width):
    count = width // 2
    exponents = jnp.arange(count, dtype=jnp.float32) * (2.0 / width)
    freqs = jnp.power(jnp.float32(rope_base), -exponents)
    angles = positions.astype(jnp.float32)[:, None] * freqs[None, :]
    cosine = jnp.cos(angles)
    sine = jnp.sin(angles)
    return (jnp.concatenate([cosine, cosine], axis=1), jnp.concatenate([sine, sine], axis=1))


def rotate(values, cosine, sine):
    count = values.shape[-1] // 2
    turned = jnp.concatenate([-values[..., count:], values[..., :count]], axis=-1)
    return values * cosine + turned * sine


def rotate_back(grads, cosine, sine):
    count = grads.shape[-1] // 2
    scaled = grads * sine
    turned = jnp.concatenate([scaled[..., count:], -scaled[..., :count]], axis=-1)
    return grads * cosine + turned


def rms_back(grad_normed, values, scale, gain):
    gained = grad_normed * gain
    gain_grad = jnp.sum(grad_normed * values * scale, axis=0)
    value_grad = scale * gained - values * (scale * scale * scale) * jnp.mean(
        gained * values, axis=1, keepdims=True
    )
    return (value_grad, gain_grad)


EVERY = ("dp", "context", "experts")
INNER = EVERY[1:]
NT = (((1,), (1,)), ((), ()))
TN = (((0,), (0,)), ((), ()))


def mm(left, right, dims=None):
    if dims is None:
        return jnp.dot(left, right, preferred_element_type=jnp.float32)
    return lax.dot_general(left, right, dims, preferred_element_type=jnp.float32)


def gate(*values):
    return lax.optimization_barrier(values)


def swap(values, axis, mask):
    count = lax.axis_size(axis)
    return lax.ppermute(values, axis, [(i, i ^ mask) for i in range(count)])


def masks_of(axis):
    count = lax.axis_size(axis)
    return [1 << bit for bit in range(count.bit_length() - 1)]


def cube_gather(values, axis):
    held = {0: values}
    for mask in reversed(masks_of(axis)):
        keys = sorted(held)
        rows = values.shape[0]
        got = swap(jnp.concatenate([held[key] for key in keys], axis=0), axis, mask)
        for at, key in enumerate(keys):
            held[key | mask] = got[at * rows : (at + 1) * rows]
    return jnp.concatenate([held[key] for key in sorted(held)], axis=0)


def cube_scatter(values, axis):
    count = lax.axis_size(axis)
    rows = values.shape[0] // count
    held = {key: values[key * rows : (key + 1) * rows] for key in range(count)}
    for mask in masks_of(axis):
        kept = [key for key in sorted(held) if not key & mask]
        sent = jnp.concatenate([held[key | mask] for key in kept], axis=0)
        got = swap(sent.astype(jnp.bfloat16), axis, mask).astype(jnp.float32)
        held = {
            key: held[key].astype(jnp.float32) + got[at * rows : (at + 1) * rows]
            for at, key in enumerate(kept)
        }
    return held[0]


def bits_of(axes):
    return [(axis, mask) for axis in axes for mask in reversed(masks_of(axis))]


def bit_here(axis, mask):
    return (lax.axis_index(axis) // mask) % 2


def ordered_gather(values, axes):
    bits = bits_of(axes)
    shape = values.shape
    for at, (axis, mask) in enumerate(bits):
        got = swap(values, axis, mask)
        values = jnp.where(
            bit_here(axis, mask) == 0,
            jnp.stack([values, got], axis=at),
            jnp.stack([got, values], axis=at),
        )
    return values.reshape(-1, *shape[1:])


def scatter_stage(values, bits, stage, dtype):
    at = bits.index(stage)
    mine = bit_here(*stage)
    kept = lax.dynamic_index_in_dim(values, mine, at, keepdims=False)
    sent = lax.dynamic_index_in_dim(values, 1 - mine, at, keepdims=False)
    got = swap(sent.astype(jnp.bfloat16), *stage)
    total = kept.astype(jnp.float32) + got.astype(jnp.float32)
    return total.astype(dtype), bits[:at] + bits[at + 1 :]


def split_bits(values, bits):
    return values.reshape([2] * len(bits) + [-1, values.shape[-1]])


def ordered_scatter(values, axes, stages, dtype=jnp.float32):
    bits = bits_of(axes)
    values = split_bits(values, bits)
    for stage in stages:
        values, bits = scatter_stage(values, bits, stage, dtype)
    return values


def sum_everywhere(values):
    for axis in ("experts", "context", "dp"):
        for mask in masks_of(axis):
            values = values + swap(values, axis, mask)
    return values


def join_dp(values, other, axis):
    first = lax.axis_index("dp") == 0
    return jnp.where(
        first,
        jnp.concatenate([values, other], axis=axis),
        jnp.concatenate([other, values], axis=axis),
    )


def pick_rows(take, parts, width):
    sources, capacity, rows_dev = take.shape
    per = 4
    wide = [part.shape[1] for part in parts]

    def body(take_ref, *refs):
        out_ref = refs[-1]
        for one in range(per):
            start = 0
            for ref in refs[:-1]:
                span = min(ref.shape[1], width - start)
                out_ref[one * capacity : (one + 1) * capacity, start : start + span] = mm(
                    take_ref[one], ref[one * rows_dev : (one + 1) * rows_dev, :span]
                ).astype(jnp.bfloat16)
                start += span

    return pl.pallas_call(
        body,
        grid=(sources // per,),
        in_specs=[pl.BlockSpec((per, capacity, rows_dev), lambda s: (s, 0, 0))]
        + [pl.BlockSpec((per * rows_dev, size), lambda s: (s, 0)) for size in wide],
        out_specs=pl.BlockSpec((per * capacity, width), lambda s: (s, 0)),
        out_shape=jax.ShapeDtypeStruct((sources * capacity, width), jnp.bfloat16),
        compiler_params=pltpu.CompilerParams(vmem_limit_bytes=40 << 20),
        cost_estimate=pl.CostEstimate(
            flops=2 * sources * capacity * rows_dev * width,
            bytes_accessed=2 * sources * (rows_dev + capacity) * width,
            transcendentals=0,
        ),
        name="pick",
    )(take, *parts)


def place_rows(take, values, extra, widths):
    sources, capacity, rows_dev = take.shape
    per = 4
    inputs = [values] if extra is None else [values, extra]
    shapes = list(widths)
    if extra is not None:
        shapes[-1] += extra.shape[1]

    def body(take_ref, *refs):
        ins, outs = refs[: len(inputs)], refs[len(inputs) :]
        for one in range(per):
            slots = slice(one * capacity, (one + 1) * capacity)
            rows = slice(one * rows_dev, (one + 1) * rows_dev)
            start = 0
            for ref, span in zip(outs, widths):
                ref[rows, :span] = mm(
                    take_ref[one], ins[0][slots, start : start + span], TN
                ).astype(jnp.bfloat16)
                start += span
            if extra is not None:
                outs[-1][rows, widths[-1] :] = mm(take_ref[one], ins[1][slots, :], TN).astype(
                    jnp.bfloat16
                )

    return pl.pallas_call(
        body,
        grid=(sources // per,),
        in_specs=[pl.BlockSpec((per, capacity, rows_dev), lambda s: (s, 0, 0))]
        + [pl.BlockSpec((per * capacity, one.shape[1]), lambda s: (s, 0)) for one in inputs],
        out_specs=[pl.BlockSpec((per * rows_dev, size), lambda s: (s, 0)) for size in shapes],
        out_shape=[
            jax.ShapeDtypeStruct((sources * rows_dev, size), jnp.bfloat16) for size in shapes
        ],
        compiler_params=pltpu.CompilerParams(vmem_limit_bytes=40 << 20),
        cost_estimate=pl.CostEstimate(
            flops=2 * sources * capacity * rows_dev * sum(shapes),
            bytes_accessed=2 * sources * (rows_dev + capacity) * sum(shapes),
            transcendentals=0,
        ),
        name="place",
    )(take, *inputs)


def gated_parts(gate, upper, act_grad):
    sig = jax.nn.sigmoid(gate)
    act = (gate * sig * upper).astype(jnp.bfloat16)
    pre_grad = jnp.concatenate(
        [act_grad * upper * sig * (1.0 + gate * (1.0 - sig)), act_grad * gate * sig], axis=1
    ).astype(jnp.bfloat16)
    return act, pre_grad


def attend_fwd_body(scale, qn_ref, qr_ref, kv_ref, kr_ref, qp_ref, kp_ref, out_ref, lse_ref):
    scores = mm(qn_ref[...], kv_ref[:, :NOPE], NT) + mm(qr_ref[0], kr_ref[...], NT)
    scores = jnp.where(kp_ref[...] <= qp_ref[...], scores * scale, masked_value)
    top = jnp.max(scores, axis=1, keepdims=True)
    weights = jnp.exp(scores - top)
    total = jnp.sum(weights, axis=1, keepdims=True)
    out = mm(weights.astype(jnp.bfloat16), kv_ref[:, NOPE:])
    out_ref[...] = (out / total).astype(jnp.bfloat16)
    lse_ref[0] = top + jnp.log(total)


def attend_fwd(q_nope, q_rope, keyvals, rope_keys, q_pos, k_pos, scale):
    heads, rows, rope = q_rope.shape
    keys = keyvals.shape[0]
    tile = min(rows, 256)
    return pl.pallas_call(
        lambda *refs: attend_fwd_body(scale, *refs),
        grid=(heads, rows // tile),
        in_specs=[
            pl.BlockSpec((tile, NOPE), lambda h, i: (i, h)),
            pl.BlockSpec((1, tile, rope), lambda h, i: (h, i, 0)),
            pl.BlockSpec((keys, NOPE + VDIM), lambda h, i: (0, h)),
            pl.BlockSpec((keys, rope), lambda h, i: (0, 0)),
            pl.BlockSpec((tile, 1), lambda h, i: (i, 0)),
            pl.BlockSpec((1, keys), lambda h, i: (0, 0)),
        ],
        out_specs=[
            pl.BlockSpec((tile, VDIM), lambda h, i: (i, h)),
            pl.BlockSpec((1, tile, 1), lambda h, i: (h, i, 0)),
        ],
        out_shape=[
            jax.ShapeDtypeStruct((rows, heads * VDIM), jnp.bfloat16),
            jax.ShapeDtypeStruct((heads, rows, 1), jnp.float32),
        ],
        compiler_params=pltpu.CompilerParams(vmem_limit_bytes=60 << 20),
        cost_estimate=pl.CostEstimate(
            flops=2 * heads * rows * keys * (NOPE + rope + VDIM),
            bytes_accessed=4 * keys * heads * (NOPE + VDIM),
            transcendentals=heads * rows * keys,
        ),
        name="af",
    )(q_nope, q_rope, keyvals, rope_keys, q_pos, k_pos)


def attend_bwd_body(
    scale,
    qn_ref,
    qr_ref,
    kv_ref,
    kr_ref,
    qp_ref,
    kp_ref,
    out_ref,
    grad_ref,
    lse_ref,
    dqn_ref,
    dqr_ref,
    dkv_ref,
    dkr_ref,
    dk_sum,
    dv_sum,
    dr_sum,
):
    head, tile = pl.program_id(1), pl.program_id(2)
    tiles = pl.num_programs(2)
    grad = grad_ref[...]
    q_nope, q_rope = qn_ref[...], qr_ref[0]
    keys, values = kv_ref[:, :NOPE], kv_ref[:, NOPE:]
    scores = mm(q_nope, keys, NT) + mm(q_rope, kr_ref[...], NT)
    probs = jnp.exp(scores * scale - lse_ref[0])
    probs = jnp.where(kp_ref[...] <= qp_ref[...], probs, 0.0)
    delta = jnp.sum(
        out_ref[...].astype(jnp.float32) * grad.astype(jnp.float32), axis=1, keepdims=True
    )
    score_grad = (probs * (mm(grad, values, NT) - delta)).astype(jnp.bfloat16)
    dqn_ref[0] = scale * mm(score_grad, keys)
    dqr_ref[0, 0] = scale * mm(score_grad, kr_ref[...])
    key_part = mm(score_grad, q_nope, TN)
    value_part = mm(probs.astype(jnp.bfloat16), grad, TN)
    rope_part = mm(score_grad, q_rope, TN)

    @pl.when(tile == 0)
    def _():
        dk_sum[...] = key_part
        dv_sum[...] = value_part

    @pl.when(tile > 0)
    def _():
        dk_sum[...] += key_part
        dv_sum[...] += value_part

    @pl.when((tile == 0) & (head == 0))
    def _():
        dr_sum[...] = rope_part

    @pl.when((tile > 0) | (head > 0))
    def _():
        dr_sum[...] += rope_part

    @pl.when(tile == tiles - 1)
    def _():
        dkv_ref[:, :NOPE] = (scale * dk_sum[...]).astype(jnp.bfloat16)
        dkv_ref[:, NOPE:] = dv_sum[...].astype(jnp.bfloat16)

    @pl.when((tile == tiles - 1) & (head == pl.num_programs(1) - 1))
    def _():
        dkr_ref[...] = (scale * dr_sum[...]).astype(jnp.bfloat16)


def attend_bwd(q_nope, q_rope, keyvals, rope_keys, q_pos, k_pos, attended, grad, lse, scale):
    heads, rows, rope = q_rope.shape
    keys = keyvals.shape[0]
    tile = min(rows, 256)
    chunk = min(keys, 2048)
    chunks = keys // chunk
    dqn, dqr, dkv, dkr = pl.pallas_call(
        lambda *refs: attend_bwd_body(scale, *refs),
        grid=(chunks, heads, rows // tile),
        in_specs=[
            pl.BlockSpec((tile, NOPE), lambda c, h, i: (i, h)),
            pl.BlockSpec((1, tile, rope), lambda c, h, i: (h, i, 0)),
            pl.BlockSpec((chunk, NOPE + VDIM), lambda c, h, i: (c, h)),
            pl.BlockSpec((chunk, rope), lambda c, h, i: (c, 0)),
            pl.BlockSpec((tile, 1), lambda c, h, i: (i, 0)),
            pl.BlockSpec((1, chunk), lambda c, h, i: (0, c)),
            pl.BlockSpec((tile, VDIM), lambda c, h, i: (i, h)),
            pl.BlockSpec((tile, VDIM), lambda c, h, i: (i, h)),
            pl.BlockSpec((1, tile, 1), lambda c, h, i: (h, i, 0)),
        ],
        out_specs=[
            pl.BlockSpec((1, tile, NOPE), lambda c, h, i: (c, i, h)),
            pl.BlockSpec((1, 1, tile, rope), lambda c, h, i: (c, h, i, 0)),
            pl.BlockSpec((chunk, NOPE + VDIM), lambda c, h, i: (c, h)),
            pl.BlockSpec((chunk, rope), lambda c, h, i: (c, 0)),
        ],
        out_shape=[
            jax.ShapeDtypeStruct((chunks, rows, heads * NOPE), jnp.float32),
            jax.ShapeDtypeStruct((chunks, heads, rows, rope), jnp.float32),
            jax.ShapeDtypeStruct((keys, heads * (NOPE + VDIM)), jnp.bfloat16),
            jax.ShapeDtypeStruct((keys, rope), jnp.bfloat16),
        ],
        scratch_shapes=[
            pltpu.VMEM((chunk, NOPE), jnp.float32),
            pltpu.VMEM((chunk, VDIM), jnp.float32),
            pltpu.VMEM((chunk, rope), jnp.float32),
        ],
        compiler_params=pltpu.CompilerParams(vmem_limit_bytes=60 << 20),
        cost_estimate=pl.CostEstimate(
            flops=2 * heads * rows * keys * (3 * NOPE + 3 * rope + 2 * VDIM),
            bytes_accessed=8 * keys * heads * (NOPE + VDIM),
            transcendentals=heads * rows * keys,
        ),
        name="ab",
    )(q_nope, q_rope, keyvals, rope_keys, q_pos, k_pos, attended, grad, lse)
    return jnp.sum(dqn, axis=0), jnp.sum(dqr, axis=0), dkv, dkr


def layer(
    layer_input,
    cotangent,
    routes,
    span_order,
    attn_gain,
    query_proj,
    latent_proj,
    latent_gain,
    expand_proj,
    output_proj,
    moe_gain,
    router_proj,
    shared_in,
    shared_out,
    expert_in,
    expert_out,
):
    place_dp = lax.axis_index("dp")
    place_context = lax.axis_index("context")
    place_experts = lax.axis_index("experts")
    count_dp = lax.axis_size("dp")
    count_context = lax.axis_size("context")
    count_experts = lax.axis_size("experts")
    own_in = layer_input[0]
    own_cot = cotangent[0]
    rows_dev = own_in.shape[0]
    sources = count_dp * count_context * count_experts
    heads = query_proj.shape[1] // (NOPE + ROPE)
    experts = router_proj.shape[1]
    shared_width = shared_out.shape[0]
    width = expert_out.shape[1]
    score_scale = 1.0 / math.sqrt(NOPE + ROPE)

    span_rows = count_experts * rows_dev
    total_rows = span_rows * count_context
    half = span_rows // 2
    width_dp = D // count_dp
    near = place_dp * width_dp
    far = (1 - place_dp) * width_dp

    names = jnp.arange(experts, dtype=jnp.int32)
    route_code = jnp.pad(routes[0], ((0, 0), (0, 128 - TOPK))).astype(jnp.bfloat16)
    all_routes = ordered_gather(route_code, EVERY)
    all_routes = all_routes[:, :TOPK].astype(jnp.int32)
    tokens = sources * rows_dev
    piece = min(tokens, 4096)
    all_cot = lax.all_gather(own_cot, EVERY, axis=0, tiled=True)

    small = jnp.concatenate([attn_gain, latent_gain, moe_gain, router_proj.reshape(-1)])
    cuts = [attn_gain.size, latent_gain.size, moe_gain.size, router_proj.size]
    starts = [sum(cuts[:i]) for i in range(4)]
    small = join_dp(small[None], swap(small, "dp", 1)[None], 0)
    attn_gain, latent_gain, moe_gain, router_flat = (
        small[:, start : start + size].reshape(-1) for start, size in zip(starts, cuts)
    )
    router_proj = router_flat.reshape(-1, experts)
    attn_gain, latent_gain, moe_gain = (
        gain.astype(jnp.float32) for gain in (attn_gain, latent_gain, moe_gain)
    )

    inputs = own_in.astype(jnp.float32)
    scale_one = lax.rsqrt(jnp.mean(inputs * inputs, axis=1, keepdims=True) + eps_norm)
    own_normed = (inputs * scale_one * attn_gain).astype(jnp.bfloat16)
    latent_shard = latent_proj.T
    far_normed = swap(lax.dynamic_slice_in_dim(own_normed, far, width_dp, 1), "dp", 1)
    far_part = mm(far_normed, latent_shard, NT)
    compressed = mm(
        lax.dynamic_slice_in_dim(own_normed, near, width_dp, 1), latent_shard, NT
    ) + swap(far_part, "dp", 1)

    span_in = cube_gather(own_in, "experts")
    query_shard, far_normed = gate(query_proj, far_normed)
    query_other = swap(query_shard, "dp", 1)
    expand_shard, query_other = gate(expand_proj, query_other)
    expand_other = swap(expand_shard, "dp", 1)
    output_shard, expand_other = gate(output_proj, expand_other)
    output_other = swap(output_shard, "dp", 1)
    shared_shard, down_shard, latent_late, output_other = gate(
        shared_in.transpose(1, 2, 0).reshape(2 * shared_width, width_dp),
        shared_out,
        latent_shard,
        output_other,
    )
    shared_other = swap(shared_shard, "dp", 1)
    down_other = swap(down_shard, "dp", 1)
    latent_other = swap(latent_late, "dp", 1)
    query_proj = join_dp(query_shard, query_other, 0)
    expand_proj = join_dp(expand_shard, expand_other, 0)
    output_proj = join_dp(output_shard, output_other, 1)
    shared_in = join_dp(shared_shard, shared_other, 1)
    shared_out = join_dp(down_shard, down_other, 1)
    latent_proj = join_dp(latent_late, latent_other, 1)

    order = lax.dynamic_slice_in_dim(span_order, 2 * place_context, 2, 0)
    offsets = jnp.arange(rows_dev, dtype=jnp.int32)
    members = jnp.arange(count_experts, dtype=jnp.int32) ^ place_experts
    span_places = (members[:, None] * rows_dev + offsets[None, :]).reshape(span_rows)
    positions = (
        jnp.where(span_places < half, order[0], order[1]) * half + span_places % half
    )
    key_positions = (
        span_order[:, None] * half + jnp.arange(half, dtype=jnp.int32)[None, :]
    ).reshape(1, total_rows)
    cosine, sine = rope_tables(positions, ROPE)
    own_cosine, own_sine = cosine[:rows_dev], sine[:rows_dev]

    latent = compressed[:, :RANK]
    scale_latent = lax.rsqrt(jnp.mean(latent * latent, axis=1, keepdims=True) + eps_norm)
    latent_normed = (latent * scale_latent * latent_gain).astype(jnp.bfloat16)
    key_rope = rotate(compressed[:, RANK:], own_cosine, own_sine).astype(jnp.bfloat16)
    keys_all = ordered_gather(jnp.concatenate([latent_normed, key_rope], axis=1), INNER)
    latent_all, rope_all = keys_all[:, :RANK], keys_all[:, RANK:]

    span_float = span_in.astype(jnp.float32)
    scale_span = lax.rsqrt(jnp.mean(span_float * span_float, axis=1, keepdims=True) + eps_norm)
    normed = (span_float * scale_span * attn_gain).astype(jnp.bfloat16)
    query_raw = mm(normed, query_proj)
    query_raw = query_raw.reshape(span_rows, heads, NOPE + ROPE)
    q_nope = query_raw[:, :, :NOPE].reshape(span_rows, heads * NOPE).astype(jnp.bfloat16)
    q_rope = (
        rotate(query_raw[:, :, NOPE:], cosine[:, None, :], sine[:, None, :])
        .transpose(1, 0, 2)
        .astype(jnp.bfloat16)
    )
    keyvals = mm(latent_all, expand_proj).astype(jnp.bfloat16)
    q_pos = positions[:, None]
    attended, lse = attend_fwd(
        q_nope, q_rope, keyvals, rope_all, q_pos, key_positions, score_scale
    )
    mixed = mm(attended, output_proj)
    hidden = inputs + cube_scatter(mixed, "experts")
    scale_two = lax.rsqrt(jnp.mean(hidden * hidden, axis=1, keepdims=True) + eps_norm)
    hidden_normed = (hidden * scale_two * moe_gain).astype(jnp.bfloat16)

    gates = jax.nn.sigmoid(mm(hidden_normed, router_proj))
    picked = jnp.any(routes[0][:, :, None] == names[None, None, :], axis=1)
    chosen = jnp.where(picked, gates, 0.0)
    chosen_total = jnp.sum(chosen, axis=1, keepdims=True)
    route_weights = route_scale * chosen / chosen_total
    weights_high = route_weights.astype(jnp.bfloat16)
    weights_low = (route_weights - weights_high.astype(jnp.float32)).astype(jnp.bfloat16)
    code_width = -(-2 * experts // 128) * 128
    all_normed = lax.all_gather(
        jnp.concatenate(
            [
                hidden_normed,
                weights_high,
                weights_low,
                jnp.zeros((rows_dev, code_width - 2 * experts), jnp.bfloat16),
            ],
            axis=1,
        ),
        EVERY,
        axis=0,
        tiled=True,
    )

    capacity = rows_dev * TOPK * 4 // (3 * experts)
    name = place_context * count_experts + place_experts
    lower = (jnp.arange(rows_dev)[:, None] <= jnp.arange(rows_dev)[None, :]).astype(jnp.bfloat16)
    slots = jnp.arange(capacity, dtype=jnp.int32)
    hit = jnp.any(all_routes == name, axis=1).reshape(sources, rows_dev)
    ranks = mm(hit.astype(jnp.bfloat16), lower).astype(jnp.int32) - 1
    take_mask = hit[:, None, :] & (ranks[:, None, :] == slots[None, :, None])
    take = take_mask.astype(jnp.bfloat16)
    gate_up = expert_in[0].transpose(1, 2, 0).reshape(2 * width, D)
    down = expert_out[0]
    grads = pick_rows(take, [all_cot], D)
    bare_grad, all_normed = gate(mm(grads, down, NT), all_normed)

    all_codes = all_normed[:, D:].astype(jnp.float32)
    code_names = jnp.arange(code_width, dtype=jnp.int32)
    weight = jnp.sum(
        jnp.where(
            (code_names == name)[None, :] | (code_names == name + experts)[None, :], all_codes, 0.0
        ),
        axis=1,
    ).reshape(sources, rows_dev)
    slot_weight = jnp.sum(
        jnp.where(take_mask, weight[:, None, :], 0.0), axis=2
    ).reshape(sources * capacity, 1)
    rows = pick_rows(take, [all_normed], D)
    pre = mm(rows, gate_up, NT)
    act, pre_grad = gated_parts(pre[:, :width], pre[:, width:], bare_grad * slot_weight)
    weight_grad = jnp.sum(act.astype(jnp.float32) * bare_grad, axis=1, keepdims=True)
    act_weighted = (act.astype(jnp.float32) * slot_weight).astype(jnp.bfloat16)
    backs = mm(pre_grad, gate_up).astype(jnp.bfloat16)
    high = weight_grad.astype(jnp.bfloat16).astype(jnp.float32)
    back_width = -(-2 * count_dp * experts // 128) * 128
    columns = jnp.arange(back_width, dtype=jnp.int32)[None, :]
    column = place_dp * experts + name
    code = jnp.where(columns == column, high, 0.0) + jnp.where(
        columns == column + count_dp * experts, weight_grad - high, 0.0
    )
    side = D // 2

    def scatter_every(values):
        return lax.psum_scatter(values, EVERY, scatter_dimension=0, tiled=True)

    code = code.astype(jnp.bfloat16)
    if tokens > piece:
        (back,) = place_rows(take, backs[:, :side], None, (side,))
        back, backs, code = gate(scatter_every(back), backs, code)
        (other,) = place_rows(take, backs[:, side:], code, (D - side,))
        back = jnp.concatenate([back, scatter_every(other)], axis=1)
    else:
        (back,) = place_rows(take, backs, code, (D,))
        back, all_normed, all_cot, pre_grad, rows, act_weighted, grads = gate(
            back, all_normed, all_cot, pre_grad, rows, act_weighted, grads
        )
        back = scatter_every(back)

    span_start = (place_dp * count_context + place_context) * span_rows

    def span_of(values):
        return jnp.concatenate(
            [
                lax.dynamic_slice_in_dim(
                    values, span_start + (place_experts ^ one) * rows_dev, rows_dev, 0
                )
                for one in range(count_experts)
            ],
            axis=0,
        )

    def shared_parts(normed_piece, cot_piece):
        shared_pre = mm(normed_piece, shared_in, NT)
        return gated_parts(
            shared_pre[:, :shared_width],
            shared_pre[:, shared_width:],
            mm(cot_piece, shared_out, NT),
        )

    if tokens > piece:
        all_normed, all_cot, back = gate(all_normed, all_cot, back)
        span_act, span_pre_grad = shared_parts(span_of(all_normed)[:, :D], span_of(all_cot))
        span_act, span_pre_grad, all_normed, all_cot = gate(
            span_act, span_pre_grad, all_normed, all_cot
        )
    shared_in_grad, shared_out_grad = 0.0, 0.0
    for start in range(0, tokens, piece):
        normed_piece = all_normed[start : start + piece, :D]
        cot_piece = all_cot[start : start + piece]
        shared_act, shared_pre_grad = shared_parts(normed_piece, cot_piece)
        shared_in_grad += mm(
            shared_pre_grad, lax.dynamic_slice_in_dim(normed_piece, near, width_dp, 1), TN
        )
        shared_out_grad += mm(
            shared_act, lax.dynamic_slice_in_dim(cot_piece, near, width_dp, 1), TN
        )
        if tokens > piece:
            shared_in_grad, shared_out_grad, all_normed, all_cot = gate(
                shared_in_grad, shared_out_grad, all_normed, all_cot
            )
        else:
            span_act, span_pre_grad = span_of(shared_act), span_of(shared_pre_grad)

    shared_sum = cube_scatter(
        jnp.concatenate(
            [
                mm(span_act, shared_out).astype(jnp.bfloat16),
                mm(span_pre_grad, shared_in).astype(jnp.bfloat16),
            ],
            axis=1,
        ),
        "experts",
    )
    expert_in_grad = mm(pre_grad, rows, TN)
    expert_out_grad = mm(act_weighted, grads, TN)
    back, shared_sum, shared_in_grad, shared_out_grad, expert_in_grad, expert_out_grad = gate(
        back, shared_sum, shared_in_grad, shared_out_grad, expert_in_grad, expert_out_grad
    )
    shared_in_grad = shared_in_grad.reshape(2, shared_width, width_dp).transpose(2, 0, 1)
    expert_in_grad = expert_in_grad.reshape(2, width, D).transpose(2, 0, 1)[None]
    expert_out_grad = expert_out_grad[None]
    back = back.astype(jnp.float32)

    codes = back[:, D : D + 2 * count_dp * experts].reshape(rows_dev, 2 * count_dp, experts)
    weight_grad = jnp.sum(codes, axis=1)
    chosen_grad = route_scale * weight_grad / chosen_total - route_scale * jnp.sum(
        weight_grad * chosen, axis=1, keepdims=True
    ) / (chosen_total * chosen_total)
    logit_grad = jnp.where(picked, chosen_grad * gates * (1.0 - gates), 0.0)
    normed_grad = (
        back[:, :D]
        + shared_sum[:, D:]
        + jnp.dot(
            logit_grad, router_proj.astype(jnp.float32).T, precision=lax.Precision.HIGHEST
        )
    )
    norm_part, moe_gain_grad = rms_back(normed_grad, hidden, scale_two, moe_gain)
    hidden_grad = own_cot.astype(jnp.float32) + norm_part
    outgoing, act_weighted = gate(hidden_grad.astype(jnp.bfloat16), act_weighted)
    hidden_round = cube_gather(outgoing, "experts")
    results = mm(act_weighted, down).astype(jnp.bfloat16)
    every_bits = bits_of(EVERY)
    inner = [bit for bit in every_bits if bit[0] == "experts"][::-1]
    along = [bit for bit in every_bits if bit[0] == "context"][::-1]
    across = [bit for bit in every_bits if bit[0] == "dp"]
    orders = (
        inner[:1] + inner[1:] + across + along,
        inner[:1] + along + across + inner[1:],
    )
    if tokens > piece:
        (forward_rows,) = place_rows(take, results, None, (D,))
        routed = scatter_every(forward_rows)
    else:
        halves = []
        for part, values in enumerate(place_rows(take, results, None, (side, D - side))):
            halves.append(
                scatter_stage(
                    split_bits(values, every_bits), every_bits, orders[part][0], jnp.bfloat16
                )
            )
        hidden_round, first_half, second_half = gate(hidden_round, halves[0][0], halves[1][0])
        routed = []
        for part, values in enumerate((first_half, second_half)):
            bits = halves[part][1]
            for stage in orders[part][1:]:
                values, bits = scatter_stage(values, bits, stage, jnp.bfloat16)
            routed.append(values)
        routed = jnp.concatenate(routed, axis=1)

    def sum_heads(values):
        kept = lax.dynamic_slice_in_dim(values, near, width_dp, 0)
        sent = lax.dynamic_slice_in_dim(values, far, width_dp, 0)
        got = swap(sent.astype(jnp.bfloat16), "dp", 1)
        kept = (kept + got.astype(jnp.float32)).astype(jnp.bfloat16)
        return lax.psum_scatter(kept, "context", scatter_dimension=0, tiled=True)

    def full_heads(values):
        return lax.all_gather(values, "context", axis=0, tiled=True).astype(jnp.float32)

    attended_grad = mm(hidden_round, output_proj, NT).astype(jnp.bfloat16)
    output_part = sum_heads(mm(hidden_round, attended, TN))
    dq_nope, dq_rope, dkv, dkr = attend_bwd(
        q_nope,
        q_rope,
        keyvals,
        rope_all,
        q_pos,
        key_positions,
        attended,
        attended_grad,
        lse,
        score_scale,
    )
    dq_rope = rotate_back(dq_rope.transpose(1, 0, 2), cosine[:, None, :], sine[:, None, :])
    query_raw_grad = (
        jnp.concatenate([dq_nope.reshape(span_rows, heads, NOPE), dq_rope], axis=2)
        .reshape(span_rows, heads * (NOPE + ROPE))
        .astype(jnp.bfloat16)
    )
    head_grads = jnp.concatenate(
        [mm(normed, query_raw_grad, TN), mm(latent_all, dkv, TN).reshape(D, -1)], axis=1
    )
    head_grads, dkv, query_raw_grad = gate(head_grads, dkv, query_raw_grad)
    head_grads = sum_heads(head_grads)
    latent_outgoing = mm(dkv, expand_proj, NT).astype(jnp.bfloat16)
    latent_outgoing = jnp.concatenate([latent_outgoing, dkr], axis=1)
    latent_part = ordered_scatter(latent_outgoing, INNER, inner + along)
    input_part = cube_scatter(mm(query_raw_grad, query_proj, NT), "experts")

    latent_grad, latent_gain_grad = rms_back(
        latent_part[:, :RANK], latent, scale_latent, latent_gain
    )
    compressed_grad = jnp.concatenate(
        [latent_grad, rotate_back(latent_part[:, RANK:], own_cosine, own_sine)], axis=1
    ).astype(jnp.bfloat16)
    latent_proj_grad = mm(own_normed, compressed_grad, TN)
    latent_proj_grad = ordered_scatter(latent_proj_grad, EVERY, inner + along + across)
    latent_proj_grad = ordered_gather(latent_proj_grad.astype(jnp.bfloat16), INNER).astype(
        jnp.float32
    )
    head_grads, output_proj_grad = full_heads(head_grads), full_heads(output_part).T
    query_wide = heads * (NOPE + ROPE)
    query_proj_grad = head_grads[:, :query_wide]
    expand_grad = head_grads[:, query_wide:].reshape(RANK // count_dp, -1)

    input_normed_grad = input_part + mm(compressed_grad, latent_proj)
    first_part, attn_gain_grad = rms_back(input_normed_grad, inputs, scale_one, attn_gain)
    input_grad = hidden_grad + first_part
    router_grad = jnp.dot(
        hidden_normed.astype(jnp.float32).T, logit_grad, precision=lax.Precision.HIGHEST
    )
    early = sum_everywhere(jnp.concatenate([moe_gain_grad, router_grad.reshape(-1)]))
    late = sum_everywhere(jnp.concatenate([attn_gain_grad, latent_gain_grad]))

    def part_dp(values, start, size):
        return lax.dynamic_slice_in_dim(values, start + place_dp * size, size, 0)

    block_output = hidden + routed.astype(jnp.float32) + shared_sum[:, :D]
    return (
        block_output[None],
        input_grad[None],
        part_dp(late, 0, cuts[0]),
        query_proj_grad,
        latent_proj_grad,
        part_dp(late, D, cuts[1]),
        expand_grad,
        output_proj_grad,
        part_dp(early, 0, cuts[2]),
        part_dp(early, D, cuts[3]).reshape(-1, experts),
        shared_in_grad,
        shared_out_grad,
        expert_in_grad,
        expert_out_grad,
    )


def solution(mesh):
    return jax.shard_map(
        layer,
        mesh=mesh,
        in_specs=(
            P("dp", ("context", "experts"), None),
            P("dp", ("context", "experts"), None),
            P("dp", ("context", "experts"), None),
            P(),
            P("dp"),
            P("dp", "experts"),
            P("dp", None),
            P("dp"),
            P("dp", "experts"),
            P("experts", "dp"),
            P("dp"),
            P("dp", None),
            P("dp", None, "experts"),
            P("experts", "dp"),
            P(("context", "experts"), None, None, "dp"),
            P(("context", "experts"), "dp", None),
        ),
        out_specs=(
            P("dp", ("context", "experts"), None),
            P("dp", ("context", "experts"), None),
            P("dp"),
            P("dp", "experts"),
            P("dp", None),
            P("dp"),
            P("dp", "experts"),
            P("experts", "dp"),
            P("dp"),
            P("dp", None),
            P("dp", None, "experts"),
            P("experts", "dp"),
            P(("context", "experts"), None, None, "dp"),
            P(("context", "experts"), "dp", None),
        ),
        check_vma=False,
    )
```
